16 devices in a mesh: dp: 2 (over y, z), tp: 8 (over x, core).
Axes of the slice: x: 4, y: 2, z: 1, core: 2. Of those that a mesh axis runs over, the one named last changes fastest.
The devices are a block of a 4x4x8 slice.
Arguments:
- hidden: bfloat16 [128, 5120], P('dp'), parts along dimension 0
- cache_len: int32 [128], P('dp'), parts along dimension 0
- lin_state: float32 [128, 40, 128, 128], P('dp', 'tp'), parts along dimension 0
- k_cache: bfloat16 [128, 8, 512, 128], P('dp', 'tp'), parts along dimension 0
- v_cache: bfloat16 [128, 8, 512, 128], P('dp', 'tp'), parts along dimension 0
- norm_first: float32 [5120], replicated
- w_qkv: bfloat16 [5120, 3, 40, 128], P(None, None, 'tp')
- w_gate: bfloat16 [5120, 40, 128], P(None, 'tp')
- slopes: float32 [40], P('tp')
- out_norm: float32 [40, 128], P('tp')
- w_out_lin: bfloat16 [40, 128, 5120], P('tp')
- norm_second: float32 [5120], replicated
- w_attn: bfloat16 [5120, 8, 7, 128], P(None, 'tp')
- w_out_attn: bfloat16 [40, 128, 5120], P('tp')
- mix_alpha: float32 [2], replicated
- mix_beta: float32 [2], replicated
Outputs:
- output 1: bfloat16 [128, 5120], P('dp'), parts along dimension 0
- output 2: float32 [128, 40, 128, 128], P('dp', 'tp'), parts along dimension 0
- output 3: bfloat16 [128, 8, 512, 128], P('dp', 'tp'), parts along dimension 0
- output 4: bfloat16 [128, 8, 512, 128], P('dp', 'tp'), parts along dimension 0
There are 2 independent parts. The reference program is written for one: setup_inputs(seed, part) draws one part's arguments, and reference() takes and returns one part's arrays. A program takes and returns all parts, laid end to end along the dimension named above; an argument that names none is the same for every part.
All inputs are finite; a program needn't handle non-finite values.
Results may differ from the reference program's by a relative error of at most 0.0114051.
Values sent between devices are 32-bit elements.
A program may use at most 768 MiB of HBM per device.

```python
import math
import jax
import jax.numpy as jnp
from jax import lax

D = 5120
HEADS = 40
KV_HEADS = 8
HEAD = 128
BATCH = 64
TMAX = 512

GROUP = HEADS // KV_HEADS
WIDTH = HEADS * HEAD
LEN_MIN = TMAX // 16
EPS = 1e-5
ROPE_BASE = 10000000.0


def setup_inputs(seed: int = 0, part: int = 0) -> dict:
    shared_keys = jax.random.split(jax.random.key(seed), 11)
    own_keys = jax.random.split(jax.random.fold_in(jax.random.key(seed), part), 8)
    hidden = jax.random.normal(own_keys[0], (BATCH, D), jnp.float32).astype(jnp.bfloat16)
    cache_len = jax.random.randint(own_keys[1], (BATCH,), LEN_MIN, TMAX, jnp.int32)
    cache_len = cache_len.at[0].set(TMAX - 1).at[1].set(LEN_MIN)
    head_scale = jnp.exp(jax.random.uniform(own_keys[2], (BATCH, HEADS, 1, 1), jnp.float32, -1.0, 1.0))
    lin_state = 2.0 * head_scale * jax.random.normal(own_keys[3], (BATCH, HEADS, HEAD, HEAD), jnp.float32)
    key_scale = math.sqrt(math.log(TMAX / 32.0))
    k_cache = (key_scale * jax.random.normal(own_keys[4], (BATCH, KV_HEADS, TMAX, HEAD), jnp.float32)).astype(jnp.bfloat16)
    pos_ramp = (2.0 * jnp.arange(TMAX, dtype=jnp.float32) / TMAX - 1.0)[None, None, :, None]
    v_base = jax.random.normal(own_keys[5], (BATCH, KV_HEADS, 1, HEAD), jnp.float32)
    v_slope = jax.random.normal(own_keys[6], (BATCH, KV_HEADS, 1, HEAD), jnp.float32)
    v_noise = jax.random.normal(own_keys[7], (BATCH, KV_HEADS, TMAX, HEAD), jnp.float32)
    v_cache = (0.5 * v_base + 0.5 * v_slope * pos_ramp + v_noise).astype(jnp.bfloat16)
    norm_first = jax.random.uniform(shared_keys[0], (D,), jnp.float32, 0.5, 1.5)
    w_qkv = (jax.random.normal(shared_keys[1], (D, 3, HEADS, HEAD), jnp.float32) * D ** -0.5).astype(jnp.bfloat16)
    w_gate = (jax.random.normal(shared_keys[2], (D, HEADS, HEAD), jnp.float32) * D ** -0.5).astype(jnp.bfloat16)
    slopes = jax.random.uniform(shared_keys[3], (HEADS,), jnp.float32, 0.02, 0.3)
    out_norm = jax.random.uniform(shared_keys[4], (HEADS, HEAD), jnp.float32, 0.5, 1.5)
    w_out_lin = (jax.random.normal(shared_keys[5], (HEADS, HEAD, D), jnp.float32) * WIDTH ** -0.5).astype(jnp.bfloat16)
    norm_second = jax.random.uniform(shared_keys[6], (D,), jnp.float32, 0.5, 1.5)
    w_attn = (jax.random.normal(shared_keys[7], (D, KV_HEADS, GROUP + 2, HEAD), jnp.float32) * D ** -0.5).astype(jnp.bfloat16)
    w_out_attn = (jax.random.normal(shared_keys[8], (HEADS, HEAD, D), jnp.float32) * WIDTH ** -0.5).astype(jnp.bfloat16)
    mix_alpha = jax.random.uniform(shared_keys[9], (2,), jnp.float32, 0.5, 1.5)
    mix_beta = jax.random.uniform(shared_keys[10], (2,), jnp.float32, 0.5, 1.5)
    return dict(hidden=hidden, cache_len=cache_len, lin_state=lin_state, k_cache=k_cache, v_cache=v_cache,
                norm_first=norm_first, w_qkv=w_qkv, w_gate=w_gate, slopes=slopes, out_norm=out_norm,
                w_out_lin=w_out_lin, norm_second=norm_second, w_attn=w_attn, w_out_attn=w_out_attn,
                mix_alpha=mix_alpha, mix_beta=mix_beta)


def rms_norm(values, gain_vec):
    wide_vals = values.astype(jnp.float32)
    mean_sq = jnp.mean(wide_vals * wide_vals, axis=-1, keepdims=True)
    return wide_vals * lax.rsqrt(mean_sq + EPS) * gain_vec


def rotary(values, positions):
    rot_dim = values.shape[-1] // 2
    half_dim = rot_dim // 2
    inv_freq = ROPE_BASE ** (-2.0 * jnp.arange(half_dim, dtype=jnp.float32) / rot_dim)
    angles = positions.astype(jnp.float32)[:, None] * inv_freq[None, :]
    cosine = jnp.cos(angles)[:, None, None, :]
    sine_val = jnp.sin(angles)[:, None, None, :]
    rot_first = values[..., :half_dim]
    rot_second = values[..., half_dim:rot_dim]
    return jnp.concatenate([rot_first * cosine - rot_second * sine_val,
                            rot_second * cosine + rot_first * sine_val,
                            values[..., rot_dim:]], axis=-1)


def lightning_layer(h_first, lin_state, w_qkv, w_gate, slopes, out_norm, w_out_lin):
    proj_lin = jnp.dot(h_first, w_qkv.reshape(D, 3 * WIDTH), preferred_element_type=jnp.float32)
    proj_lin = jax.nn.silu(proj_lin).astype(jnp.bfloat16).astype(jnp.float32).reshape(BATCH, 3, HEADS, HEAD)
    query_lin = proj_lin[:, 0]
    key_lin = proj_lin[:, 1]
    value_lin = proj_lin[:, 2]
    decay_rate = jnp.exp(-slopes)[None, :, None, None]
    state_out = decay_rate * lin_state + jnp.einsum('bhk,bhv->bhkv', key_lin, value_lin)
    lin_attn = jnp.einsum('bhk,bhkv->bhv', query_lin, state_out)
    mean_sq = jnp.mean(lin_attn * lin_attn, axis=(1, 2), keepdims=True)
    normed = (lin_attn * lax.rsqrt(mean_sq + EPS) * out_norm).reshape(BATCH, WIDTH)
    gate_val = jax.nn.sigmoid(jnp.dot(h_first, w_gate.reshape(D, WIDTH), preferred_element_type=jnp.float32))
    gated_out = (normed * gate_val).astype(jnp.bfloat16)
    lin_out = jnp.dot(gated_out, w_out_lin.reshape(WIDTH, D), preferred_element_type=jnp.float32)
    return lin_out, state_out


def softmax_layer(h_second, cache_len, k_cache, v_cache, w_attn, w_out_attn):
    proj_attn = jnp.dot(h_second, w_attn.reshape(D, KV_HEADS * (GROUP + 2) * HEAD), preferred_element_type=jnp.float32)
    proj_attn = proj_attn.reshape(BATCH, KV_HEADS, GROUP + 2, HEAD)
    turned = rotary(proj_attn[:, :, :GROUP + 1], cache_len).astype(jnp.bfloat16)
    query_new = turned[:, :, :GROUP]
    key_new = turned[:, :, GROUP]
    value_new = proj_attn[:, :, GROUP + 1].astype(jnp.bfloat16)
    positions = jnp.arange(TMAX, dtype=jnp.int32)
    write_mask = (positions[None, :] == cache_len[:, None])[:, None, :, None]
    k_out = jnp.where(write_mask, key_new[:, :, None, :], k_cache)
    v_out = jnp.where(write_mask, value_new[:, :, None, :], v_cache)

    def one_row(row_args):
        query_row, key_row, value_row, length = row_args
        scores = jnp.einsum('kgc,ktc->kgt', query_row.astype(jnp.float32), key_row.astype(jnp.float32)) * HEAD ** -0.5
        scores = jnp.where(positions[None, None, :] <= length, scores, -jnp.inf)
        probs_row = jax.nn.softmax(scores, axis=-1).astype(jnp.bfloat16)
        return jnp.einsum('kgt,ktc->kgc', probs_row.astype(jnp.float32), value_row.astype(jnp.float32)).astype(jnp.bfloat16)

    attn_rows = lax.map(one_row, (query_new, k_out, v_out, cache_len))
    attn_out = jnp.dot(attn_rows.reshape(BATCH, WIDTH), w_out_attn.reshape(WIDTH, D), preferred_element_type=jnp.float32)
    return attn_out, k_out, v_out


def reference(hidden, cache_len, lin_state, k_cache, v_cache, norm_first, w_qkv, w_gate, slopes, out_norm,
              w_out_lin, norm_second, w_attn, w_out_attn, mix_alpha, mix_beta):
    h_first = rms_norm(hidden, norm_first).astype(jnp.bfloat16)
    lin_out, state_out = lightning_layer(h_first, lin_state, w_qkv, w_gate, slopes, out_norm, w_out_lin)
    mid_hidden = (mix_alpha[0] * h_first.astype(jnp.float32) + mix_beta[0] * lin_out).astype(jnp.bfloat16)
    h_second = rms_norm(mid_hidden, norm_second).astype(jnp.bfloat16)
    attn_out, k_out, v_out = softmax_layer(h_second, cache_len, k_cache, v_cache, w_attn, w_out_attn)
    hidden_out = (mix_alpha[1] * h_second.astype(jnp.float32) + mix_beta[1] * attn_out).astype(jnp.bfloat16)
    return hidden_out, state_out, k_out, v_out
```

```python
import functools

import jax
import jax.numpy as jnp
from jax import lax
from jax.experimental import pallas as pl
from jax.experimental.pallas import tpu as pltpu
from jax.sharding import PartitionSpec as P

EPS = 1e-5
ROPE_BASE = 10000000.0
MESH = pl.DeviceIdType.MESH
VMEM = pl.BlockSpec(memory_space=pltpu.VMEM)
SMEM = pl.BlockSpec(memory_space=pltpu.SMEM)
HBM = pl.BlockSpec(memory_space=pltpu.HBM)
ROWS = 8
LANES = 128


def lightning_kernel(slopes_ref, hidden_ref, norm_ref, wqkv_ref, wgate_ref, state_ref, onorm_ref, wout_ref,
                     state_out_ref, part_ref, h1_out_ref,
                     h1_ref, sq_ref, kt_ref, qt_ref, v_ref, o_ref):
    head = pl.program_id(0)
    heads = pl.num_programs(0)
    batch, width = hidden_ref.shape

    @pl.when(head == 0)
    def _():
        x = hidden_ref[...].astype(jnp.float32)
        h1 = x * lax.rsqrt(jnp.mean(x * x, axis=-1, keepdims=True) + EPS) * norm_ref[...]
        h1 = h1.astype(jnp.bfloat16)
        h1_ref[...] = h1
        h1_out_ref[...] = h1.astype(jnp.float32).reshape(h1_out_ref.shape)
        sq_ref[...] = jnp.zeros_like(sq_ref)

    def project(w):
        return jnp.dot(h1_ref[...], w, preferred_element_type=jnp.float32)

    def silu(x):
        return (x * jax.nn.sigmoid(x)).astype(jnp.bfloat16).astype(jnp.float32)

    q = silu(project(wqkv_ref[0, 0]))
    k = silu(project(wqkv_ref[1, 0]))
    v = silu(project(wqkv_ref[2, 0]))
    gate = jax.nn.sigmoid(project(wgate_ref[0]))
    v_ref[...] = v
    kt = k.T
    qt = q.T
    for i in range(batch // ROWS):
        kt_ref[i] = kt[:, i * ROWS:(i + 1) * ROWS]
        qt_ref[i] = qt[:, i * ROWS:(i + 1) * ROWS]
    decay = jnp.exp(-jnp.full((1, LANES), slopes_ref[head], jnp.float32))

    def block(i, _):
        kb, qb = kt_ref[i], qt_ref[i]
        base = pl.multiple_of(i * ROWS, ROWS)
        vb = v_ref[pl.ds(base, ROWS), :]
        outs = []
        for r in range(ROWS):
            new = decay * state_ref[base + r, 0] + kb[:, r:r + 1] * vb[r:r + 1, :]
            state_out_ref[base + r, 0] = new
            outs.append(jnp.sum(qb[:, r:r + 1] * new, axis=0, keepdims=True))
        o_ref[pl.ds(base, ROWS), :] = jnp.concatenate(outs, axis=0)
        return 0

    lax.fori_loop(0, batch // ROWS, block, 0)
    o = o_ref[...]
    sq_ref[...] += jnp.broadcast_to(jnp.sum(o * o, axis=1, keepdims=True), sq_ref.shape)
    gated = (o * onorm_ref[0] * gate).astype(jnp.bfloat16)
    tile = 1024
    for c in range(width // tile):
        cols = pl.ds(c * tile, tile)
        piece = jnp.dot(gated, wout_ref[0, :, cols], preferred_element_type=jnp.float32)
        piece = piece.reshape(batch // ROWS, ROWS, tile)

        @pl.when(head == 0)
        def _():
            part_ref[:, :, cols] = piece

        @pl.when(head > 0)
        def _():
            part_ref[:, :, cols] += piece

    @pl.when(head == heads - 1)
    def _():
        part_ref[:, :, pl.ds(width, LANES)] = sq_ref[...].reshape(batch // ROWS, ROWS, LANES)


def lightning(hidden, norm_first, w_qkv, w_gate, lin_state, slopes, out_norm, w_out_lin):
    batch, width = hidden.shape
    heads, dim = out_norm.shape
    blocks = batch // ROWS
    return pl.pallas_call(
        lightning_kernel,
        grid=(heads,),
        out_shape=(jax.ShapeDtypeStruct(lin_state.shape, jnp.float32),
                   jax.ShapeDtypeStruct((blocks, ROWS, width + LANES), jnp.float32),
                   jax.ShapeDtypeStruct((blocks, ROWS, width), jnp.float32)),
        in_specs=[
            SMEM,
            pl.BlockSpec((batch, width), lambda h: (0, 0)),
            pl.BlockSpec((1, width), lambda h: (0, 0)),
            pl.BlockSpec((3, 1, width, dim), lambda h: (0, h, 0, 0)),
            pl.BlockSpec((1, width, dim), lambda h: (h, 0, 0)),
            pl.BlockSpec((batch, 1, dim, dim), lambda h: (0, h, 0, 0)),
            pl.BlockSpec((1, 1, dim), lambda h: (h, 0, 0)),
            pl.BlockSpec((1, dim, width), lambda h: (h, 0, 0)),
        ],
        out_specs=(
            pl.BlockSpec((batch, 1, dim, dim), lambda h: (0, h, 0, 0)),
            pl.BlockSpec((blocks, ROWS, width + LANES), lambda h: (0, 0, 0)),
            pl.BlockSpec((blocks, ROWS, width), lambda h: (0, 0, 0)),
        ),
        scratch_shapes=[
            pltpu.VMEM((batch, width), jnp.bfloat16),
            pltpu.VMEM((batch, LANES), jnp.float32),
            pltpu.VMEM((blocks, dim, ROWS), jnp.float32),
            pltpu.VMEM((blocks, dim, ROWS), jnp.float32),
            pltpu.VMEM((batch, dim), jnp.float32),
            pltpu.VMEM((batch, dim), jnp.float32),
        ],
        compiler_params=pltpu.CompilerParams(vmem_limit_bytes=56 << 20),
        cost_estimate=pl.CostEstimate(flops=2 * batch * width * heads * dim * 5, transcendentals=0,
                                      bytes_accessed=2 * lin_state.size * 4 + 10 * heads * dim * width),
        name="lightning",
    )(slopes, hidden, norm_first.reshape(1, width), w_qkv.transpose(1, 2, 0, 3), w_gate.transpose(1, 0, 2),
      lin_state, out_norm.reshape(heads, 1, dim), w_out_lin)


def reduce_kernel(finish, chips, split, n_extra, part_ref, *refs):
    extra, (all_ref, own_ref), scratch = refs[:n_extra], refs[n_extra:n_extra + 2], refs[n_extra + 2:]
    pair_ref, acc_ref, up_a, up_b, up_c, down_a, down_b, down_c, gather_ref, send_sem, recv_sem = scratch
    width = part_ref.shape[2]
    out_width = gather_ref.shape[2]
    cut = out_width // 2
    me = lax.axis_index("tp")
    chip, core = me // 2, me % 2
    mate = 2 * chip + (1 - core)
    next_chip, prev_chip, far_chip = (chip + 1) % chips, (chip + chips - 1) % chips, (chip + 2) % chips
    up, down = 2 * next_chip + core, 2 * prev_chip + core

    barrier = pltpu.get_barrier_semaphore()
    for peer in (mate, up, down):
        pl.semaphore_signal(barrier, inc=1, device_id={"tp": peer}, device_id_type=MESH)
    pl.semaphore_wait(barrier, 3)

    counter = iter(range(64))

    def copy(src, dst, peer):
        i = next(counter)
        return pltpu.make_async_remote_copy(src_ref=src, dst_ref=dst, send_sem=send_sem.at[i], recv_sem=recv_sem.at[i],
                                            device_id={"tp": peer}, device_id_type=MESH)

    lo, hi = pl.ds(0, split), pl.ds(split, width - split)

    pair = [copy(part_ref.at[2 * t + (1 - core)], pair_ref.at[s], mate)
            for s, t in enumerate((far_chip, next_chip, prev_chip, chip))]
    for c in pair:
        c.start()
    pair[0].wait_recv()
    acc_ref[0] = part_ref[2 * far_chip + core] + pair_ref[0]
    far_up = copy(acc_ref.at[0, :, lo], up_a, up)
    far_down = copy(acc_ref.at[0, :, hi], down_a, down)
    far_up.start()
    far_down.start()
    pair[1].wait_recv()
    acc_ref[1] = part_ref[2 * next_chip + core] + pair_ref[1]
    near_up = copy(acc_ref.at[1, :, hi], up_b, up)
    near_up.start()
    pair[2].wait_recv()
    acc_ref[2] = part_ref[2 * prev_chip + core] + pair_ref[2]
    near_down = copy(acc_ref.at[2, :, lo], down_b, down)
    near_down.start()
    far_up.wait_recv()
    acc_ref[1, :, lo] += up_a[...]
    sum_up = copy(acc_ref.at[1, :, lo], up_c, up)
    sum_up.start()
    far_down.wait_recv()
    acc_ref[2, :, hi] += down_a[...]
    sum_down = copy(acc_ref.at[2, :, hi], down_c, down)
    sum_down.start()
    pair[3].wait_recv()
    acc_ref[3] = part_ref[me] + pair_ref[3]
    near_up.wait_recv()
    acc_ref[3, :, hi] += up_b[...]
    near_down.wait_recv()
    acc_ref[3, :, lo] += down_b[...]
    sum_up.wait_recv()
    acc_ref[3, :, lo] += up_c[...]
    sum_down.wait_recv()
    acc_ref[3, :, hi] += down_c[...]

    finish(me, acc_ref, own_ref, gather_ref, *extra)

    first, second = pl.ds(0, cut), pl.ds(cut, out_width - cut)

    def block(dev, cols):
        return gather_ref.at[dev, :, cols]

    def move(dev, cols, peer):
        return copy(block(dev, cols), block(dev, cols), peer)

    up_first, down_second = move(me, first, up), move(me, second, down)
    up_second, down_first = move(me, second, up), move(me, first, down)
    to_mate = move(me, pl.ds(0, out_width), mate)
    for c in (up_first, down_second, up_second, down_first, to_mate):
        c.start()
    sends = [to_mate]
    up_first.wait_recv()
    relay_up = move(down, first, up)
    relay_up.start()
    pass_0 = move(down, first, mate)
    pass_0.start()
    down_second.wait_recv()
    relay_down = move(up, second, down)
    relay_down.start()
    pass_1 = move(up, second, mate)
    pass_1.start()
    up_second.wait_recv()
    pass_2 = move(down, second, mate)
    pass_2.start()
    down_first.wait_recv()
    pass_3 = move(up, first, mate)
    pass_3.start()
    far = 2 * far_chip + core
    relay_up.wait_recv()
    pass_4 = move(far, first, mate)
    pass_4.start()
    relay_down.wait_recv()
    pass_5 = move(far, second, mate)
    pass_5.start()
    passes = [pass_0, pass_1, pass_2, pass_3, pass_4, pass_5]
    to_mate.wait_recv()
    for c in passes:
        c.wait_recv()
    all_ref[...] = gather_ref[...].reshape(all_ref.shape).astype(all_ref.dtype)
    for c in (pair + [far_up, far_down, near_up, near_down, sum_up, sum_down, up_first, down_second, up_second,
                      down_first, relay_up, relay_down] + sends + passes):
        c.wait_send()


def all_reduce(finish, collective_id, tp_size, part, extra, extra_specs, out_width, name):
    blocks, rows, width = part.shape
    split = (width // LANES + 1) // 2 * LANES
    chips = tp_size // 2
    f32 = jnp.float32
    return pl.pallas_call(
        functools.partial(reduce_kernel, finish, chips, split, len(extra)),
        out_shape=(jax.ShapeDtypeStruct((blocks * rows, out_width), jnp.bfloat16),
                   jax.ShapeDtypeStruct((rows, out_width), f32)),
        in_specs=[VMEM] + extra_specs,
        out_specs=(VMEM, VMEM),
        scratch_shapes=[
            pltpu.VMEM((chips, rows, width), f32),
            pltpu.VMEM((chips, rows, width), f32),
            pltpu.VMEM((rows, split), f32), pltpu.VMEM((rows, width - split), f32), pltpu.VMEM((rows, split), f32),
            pltpu.VMEM((rows, width - split), f32), pltpu.VMEM((rows, split), f32), pltpu.VMEM((rows, width - split), f32),
            pltpu.VMEM((blocks, rows, out_width), f32),
            pltpu.SemaphoreType.DMA((32,)), pltpu.SemaphoreType.DMA((32,)),
        ],
        compiler_params=pltpu.CompilerParams(collective_id=collective_id, has_side_effects=True,
                                             vmem_limit_bytes=16 << 20),
        cost_estimate=pl.CostEstimate(flops=10 ** 9, transcendentals=0, bytes_accessed=10 ** 7),
        name=name,
    )(part, *extra)


def finish_first(full_width, me, acc_ref, own_ref, gather_ref, h1_ref, norm_ref, alpha_ref, beta_ref):
    width = own_ref.shape[1]
    inv = lax.rsqrt(acc_ref[3, :, pl.ds(width, 1)] / full_width + EPS)
    lin = acc_ref[3, :, pl.ds(0, width)] * inv
    mid = (alpha_ref[0] * h1_ref[me] + beta_ref[0] * lin).astype(jnp.bfloat16).astype(jnp.float32)
    h2 = mid * lax.rsqrt(jnp.mean(mid * mid, axis=-1, keepdims=True) + EPS) * norm_ref[...]
    h2 = h2.astype(jnp.bfloat16).astype(jnp.float32)
    own_ref[...] = h2
    gather_ref[me] = h2


def finish_second(me, acc_ref, own_ref, gather_ref, h2_ref, alpha_ref, beta_ref):
    out = (alpha_ref[1] * h2_ref[...] + beta_ref[1] * acc_ref[3]).astype(jnp.bfloat16).astype(jnp.float32)
    own_ref[...] = out
    gather_ref[me] = out


def attention_kernel(len_ref, h2_ref, watt_ref, cos_ref, sina_ref, sinb_ref, k_ref, v_ref, wout_ref,
                     k_out_ref, v_out_ref, part_ref, q_ref, kn_ref, vn_ref, att_ref):
    step = pl.program_id(0)
    steps = pl.num_programs(0)
    per = k_ref.shape[0]
    batch, width = h2_ref.shape
    group = watt_ref.shape[0] - 2
    dim = watt_ref.shape[2]
    tmax = k_ref.shape[2]

    @pl.when(step == 0)
    def _():
        h2 = h2_ref[...]

        def turn(x):
            return x * cos_ref[...] + pltpu.roll(x, dim - dim // 4, 1) * sina_ref[...] + pltpu.roll(x, dim // 4, 1) * sinb_ref[...]

        q_ref[...] = jnp.zeros_like(q_ref)
        for j in range(group):
            x = jnp.dot(h2, watt_ref[j], preferred_element_type=jnp.float32)
            q_ref[:, j, :] = turn(x)
        kn_ref[...] = turn(jnp.dot(h2, watt_ref[group], preferred_element_type=jnp.float32))
        vn_ref[...] = jnp.dot(h2, watt_ref[group + 1], preferred_element_type=jnp.float32)

    sub = 16
    rows16 = lax.broadcasted_iota(jnp.int32, (sub, dim), 0)
    cols = lax.broadcasted_iota(jnp.int32, (ROWS, tmax), 1)
    scale = dim ** -0.5
    base = step * per
    for ref, out, new in ((k_ref, k_out_ref, kn_ref), (v_ref, v_out_ref, vn_ref)):
        out[...] = ref[...]
        for r in range(per):
            pos = len_ref[base + r]
            start = pl.multiple_of((pos // sub) * sub, sub)
            old = out[r, 0, pl.ds(start, sub), :].astype(jnp.float32)
            row = new[pl.ds(base + r, 1), :]
            out[r, 0, pl.ds(start, sub), :] = jnp.where(rows16 == pos - start, row, old).astype(jnp.bfloat16)
    for r in range(per):
        pos = len_ref[base + r]
        q = q_ref[base + r].astype(jnp.bfloat16)
        s = lax.dot_general(q, k_out_ref[r, 0], (((1,), (1,)), ((), ())), preferred_element_type=jnp.float32) * scale
        s = jnp.where(cols <= pos, s, -jnp.inf)
        e = jnp.exp(s - jnp.max(s, axis=1, keepdims=True))
        p = (e / jnp.sum(e, axis=1, keepdims=True)).astype(jnp.bfloat16)
        att_ref[base + r] = jnp.dot(p, v_out_ref[r, 0], preferred_element_type=jnp.float32)

    @pl.when(step == steps - 1)
    def _():
        rows = jnp.concatenate([att_ref[:, j, :] for j in range(group)], axis=1).astype(jnp.bfloat16)
        tile = 1024
        for c in range(width // tile):
            cs = pl.ds(c * tile, tile)
            piece = jnp.dot(rows, wout_ref[:, cs], preferred_element_type=jnp.float32)
            part_ref[:, :, cs] = piece.reshape(batch // ROWS, ROWS, tile)


def attention(cache_len, h2, w_attn, tables, k_cache, v_cache, w_out):
    batch, width = h2.shape
    _, _, tmax, dim = k_cache.shape
    slots = w_attn.shape[0]
    per = 8
    blocks = batch // ROWS
    cache_spec = pl.BlockSpec((per, 1, tmax, dim), lambda i: (i, 0, 0, 0))

    def whole(x):
        return pl.BlockSpec(x.shape, lambda i: (0,) * x.ndim)

    return pl.pallas_call(
        attention_kernel,
        grid=(batch // per,),
        out_shape=(jax.ShapeDtypeStruct(k_cache.shape, k_cache.dtype),
                   jax.ShapeDtypeStruct(v_cache.shape, v_cache.dtype),
                   jax.ShapeDtypeStruct((blocks, ROWS, width), jnp.float32)),
        in_specs=[SMEM, whole(h2), whole(w_attn)] + [whole(t) for t in tables] + [cache_spec, cache_spec, whole(w_out)],
        out_specs=(cache_spec, cache_spec, pl.BlockSpec((blocks, ROWS, width), lambda i: (0, 0, 0))),
        scratch_shapes=[
            pltpu.VMEM((batch, ROWS, dim), jnp.float32),
            pltpu.VMEM((batch, dim), jnp.float32),
            pltpu.VMEM((batch, dim), jnp.float32),
            pltpu.VMEM((batch, ROWS, dim), jnp.float32),
        ],
        compiler_params=pltpu.CompilerParams(vmem_limit_bytes=60 << 20),
        cost_estimate=pl.CostEstimate(flops=2 * batch * width * dim * slots * 2, transcendentals=0,
                                      bytes_accessed=4 * k_cache.size * 2),
        name="attention",
    )(cache_len, h2, w_attn, *tables, k_cache, v_cache, w_out)


def rotary_tables(cache_len, dim):
    rot = dim // 2
    half = rot // 2
    inv_freq = ROPE_BASE ** (-2.0 * jnp.arange(half, dtype=jnp.float32) / rot)
    angles = cache_len.astype(jnp.float32)[:, None] * inv_freq[None, :]
    cosine, sine = jnp.cos(angles), jnp.sin(angles)
    ones = jnp.ones((cache_len.shape[0], dim - rot), jnp.float32)
    zero = jnp.zeros_like(sine)
    return (jnp.concatenate([cosine, cosine, ones], axis=1),
            jnp.concatenate([-sine, zero, 0 * ones], axis=1),
            jnp.concatenate([zero, sine, 0 * ones], axis=1))


def solution(mesh):
    tp_size = mesh.shape['tp']
    row_spec = P('dp', None)
    cache_spec = P('dp', 'tp', None, None)
    in_specs = (row_spec, P('dp'), cache_spec, cache_spec, cache_spec, P(None), P(None, None, 'tp', None),
                P(None, 'tp', None), P('tp'), P('tp', None), P('tp', None, None), P(None),
                P(None, 'tp', None, None), P('tp', None, None), P(None), P(None))
    out_specs = (row_spec, cache_spec, cache_spec, cache_spec)

    def local_step(hidden, cache_len, lin_state, k_cache, v_cache, norm_first, w_qkv, w_gate, slopes, out_norm,
                   w_out_lin, norm_second, w_attn, w_out_attn, mix_alpha, mix_beta):
        width = hidden.shape[1]
        dim = k_cache.shape[3]
        full_width = w_out_lin.shape[0] * dim * tp_size
        tables = rotary_tables(cache_len, dim)
        state_out, part, h1 = lightning(hidden, norm_first, w_qkv, w_gate, lin_state, slopes, out_norm, w_out_lin)
        h2, h2_own = all_reduce(functools.partial(finish_first, full_width), 0, tp_size, part,
                                (h1, norm_second.reshape(1, width), mix_alpha, mix_beta), [VMEM, VMEM, SMEM, SMEM],
                                width, "reduce_first")
        w_heads = w_attn.transpose(1, 2, 0, 3).reshape(w_attn.shape[2], width, dim)
        k_out, v_out, part = attention(cache_len, h2, w_heads, tables, k_cache, v_cache,
                                       w_out_attn.reshape(w_out_attn.shape[0] * dim, width))
        hidden_out, _ = all_reduce(finish_second, 1, tp_size, part, (h2_own, mix_alpha, mix_beta), [VMEM, SMEM, SMEM],
                                   width, "reduce_second")
        return hidden_out, state_out, k_out, v_out

    return jax.shard_map(local_step, mesh=mesh, in_specs=in_specs, out_specs=out_specs, check_vma=False)
```

```python
import functools

import jax
import jax.numpy as jnp
import numpy as np
from jax import lax
from jax.experimental import pallas as pl
from jax.experimental.pallas import tpu as pltpu
from jax.sharding import PartitionSpec as P

EPS = 1e-5
ROPE_BASE = 10000000.0
MESH = pl.DeviceIdType.MESH
VMEM = pl.BlockSpec(memory_space=pltpu.VMEM)
SMEM = pl.BlockSpec(memory_space=pltpu.SMEM)
HBM = pl.BlockSpec(memory_space=pltpu.HBM)
ROWS = 8
LANES = 128


CHUNKS = 4
WINDOW = 9
SLOTS = 3


def lightning_kernel(slopes_hbm, len_hbm, freq_hbm, norm_hbm, onorm_hbm, hidden_hbm, wqkv_hbm, wgate_hbm, state_hbm, wout_hbm,
                     state_out_hbm, part_ref, h1_out_ref, table_ref, pos_ref,
                     slopes_ref, len_ref, freq_ref, norm_ref, onorm_ref, hidden_ref, wqkv_ref, wgate_ref, state_ref, wout_ref, h1_ref, sq_ref, kt_ref, qt_ref, v_ref, o_ref,
                     small_sem, w_sem, in_sem, out_sem):
    batch, width = hidden_ref.shape
    heads, dim = onorm_ref.shape
    rows = batch // CHUNKS

    def state_in(h, c):
        return pltpu.make_async_copy(state_hbm.at[pl.ds(c * rows, rows), h], state_ref.at[h % SLOTS, pl.ds(c * rows, rows)], in_sem.at[h % SLOTS, c])

    def state_out(h, c):
        return pltpu.make_async_copy(state_ref.at[h % SLOTS, pl.ds(c * rows, rows)], state_out_hbm.at[pl.ds(c * rows, rows), h],
                                     out_sem.at[h % SLOTS, c])

    small = [pltpu.make_async_copy(src, dst, small_sem.at[i])
             for i, (src, dst) in enumerate(((len_hbm, len_ref), (freq_hbm, freq_ref), (hidden_hbm, hidden_ref), (norm_hbm, norm_ref),
                                             (slopes_hbm, slopes_ref), (onorm_hbm, onorm_ref)))]
    def piece(h, j):
        if j < 3:
            return pltpu.make_async_copy(wqkv_hbm.at[j, h], wqkv_ref.at[h % 2, j], w_sem.at[h % 2, j])
        if j == 3:
            return pltpu.make_async_copy(wgate_hbm.at[h], wgate_ref.at[h % 2], w_sem.at[h % 2, 3])
        if j < 4 + CHUNKS:
            return state_in(h, j - 4)
        return pltpu.make_async_copy(wout_hbm.at[h], wout_ref.at[h % 2], w_sem.at[h % 2, 4])

    pieces = 5 + CHUNKS

    def take(h, j):
        piece(h, j).wait()
        ahead, later = (j + WINDOW) // pieces, (j + WINDOW) % pieces

        if 4 <= later < 4 + CHUNKS:
            @pl.when((h + ahead >= SLOTS) & (h + ahead < heads))
            def _():
                state_out(h + ahead - SLOTS, later - 4).wait()

        @pl.when(h + ahead < heads)
        def _():
            piece(h + ahead, later).start()

    for c in small:
        c.start()
    for i in range(WINDOW):
        piece(i // pieces, i % pieces).start()

    for c in small[:2]:
        c.wait()
    for r in range(batch):
        pos_ref[r] = jnp.full((ROWS, LANES), len_ref[r], jnp.int32)
    angle = pos_ref[:, 0, :].astype(jnp.float32) * freq_ref[...]
    cosine, sine = jnp.cos(angle), jnp.sin(angle)
    lane = lax.broadcasted_iota(jnp.int32, angle.shape, 1)
    table_ref[0] = jnp.where(lane < dim // 2, cosine, 1.0)
    table_ref[1] = jnp.where(lane < dim // 4, -sine, 0.0)
    table_ref[2] = jnp.where((lane >= dim // 4) & (lane < dim // 2), sine, 0.0)

    for c in small[2:]:
        c.wait()
    x = hidden_ref[...].astype(jnp.float32)
    h1 = x * lax.rsqrt(jnp.mean(x * x, axis=-1, keepdims=True) + EPS) * norm_ref[...]
    h1 = h1.astype(jnp.bfloat16)
    h1_ref[...] = h1
    h1_out_ref[...] = h1.astype(jnp.float32).reshape(h1_out_ref.shape)
    sq_ref[...] = jnp.zeros_like(sq_ref)
    part_ref[...] = jnp.zeros_like(part_ref)

    def silu(x):
        return (x * jax.nn.sigmoid(x)).astype(jnp.bfloat16).astype(jnp.float32)

    def one_head(head, _):
        def project(w):
            return jnp.dot(h1_ref[...], w, preferred_element_type=jnp.float32)

        take(head, 0)
        q = silu(project(wqkv_ref[head % 2, 0]))
        take(head, 1)
        k = silu(project(wqkv_ref[head % 2, 1]))
        take(head, 2)
        v = silu(project(wqkv_ref[head % 2, 2]))
        take(head, 3)
        gate = jax.nn.sigmoid(project(wgate_ref[head % 2]))
        v_ref[...] = v
        kt = k.T
        qt = q.T
        for i in range(batch // ROWS):
            kt_ref[i] = kt[:, i * ROWS:(i + 1) * ROWS]
            qt_ref[i] = qt[:, i * ROWS:(i + 1) * ROWS]
        decay = jnp.exp(-jnp.full((1, LANES), slopes_ref[head], jnp.float32))

        def block(i, _):
            kb, qb = kt_ref[i], qt_ref[i]
            base = pl.multiple_of(i * ROWS, ROWS)
            vb = v_ref[pl.ds(base, ROWS), :]
            outs = []
            for r in range(ROWS):
                new = decay * state_ref[head % SLOTS, base + r] + kb[:, r:r + 1] * vb[r:r + 1, :]
                state_ref[head % SLOTS, base + r] = new
                outs.append(jnp.sum(qb[:, r:r + 1] * new, axis=0, keepdims=True))
            o_ref[pl.ds(base, ROWS), :] = jnp.concatenate(outs, axis=0)
            return 0

        per = rows // ROWS

        for c in range(CHUNKS):
            take(head, 4 + c)
            lax.fori_loop(c * per, (c + 1) * per, block, 0)
            state_out(head, c).start()
        o = o_ref[...]
        sq_ref[...] += jnp.broadcast_to(jnp.sum(o * o, axis=1, keepdims=True), sq_ref.shape)
        gated = (o * onorm_ref[pl.ds(head, 1), :] * gate).astype(jnp.bfloat16)
        take(head, pieces - 1)
        tile = 1024
        for c in range(width // tile):
            cols = pl.ds(c * tile, tile)
            piece = jnp.dot(gated, wout_ref[head % 2, :, cols], preferred_element_type=jnp.float32)
            part_ref[:, :, cols] += piece.reshape(batch // ROWS, ROWS, tile)
        return 0

    lax.fori_loop(0, heads, one_head, 0)
    part_ref[:, :, pl.ds(width, LANES)] = sq_ref[...].reshape(batch // ROWS, ROWS, LANES)
    for h in range(max(heads - SLOTS, 0), heads):
        for c in range(CHUNKS):
            state_out(h, c).wait()


def in_hbm(x):
    return pltpu.with_memory_space_constraint(x, pltpu.HBM)


def in_vmem(x):
    return pltpu.with_memory_space_constraint(x, pltpu.VMEM)


def lightning(hidden, cache_len, freq, norm_first, w_qkv, w_gate, lin_state, slopes, out_norm, w_out_lin):
    batch, width = hidden.shape
    heads, dim = out_norm.shape
    blocks = batch // ROWS
    f32, bf16 = jnp.float32, jnp.bfloat16
    return pl.pallas_call(
        lightning_kernel,
        out_shape=(pltpu.HBM(lin_state.shape, f32),
                   pltpu.VMEM((blocks, ROWS, width + LANES), f32),
                   pltpu.VMEM((blocks, ROWS, width), f32),
                   pltpu.VMEM((3, batch, dim), f32),
                   pltpu.VMEM((batch, ROWS, LANES), jnp.int32)),
        in_specs=[HBM] * 10,
        out_specs=(HBM, VMEM, VMEM, VMEM, VMEM),
        scratch_shapes=[
            pltpu.SMEM((heads,), f32),
            pltpu.SMEM((batch,), jnp.int32),
            pltpu.VMEM((1, dim), f32),
            pltpu.VMEM((1, width), f32),
            pltpu.VMEM((heads, dim), f32),
            pltpu.VMEM((batch, width), bf16),
            pltpu.VMEM((2, 3, width, dim), bf16),
            pltpu.VMEM((2, width, dim), bf16),
            pltpu.VMEM((SLOTS, batch, dim, dim), f32),
            pltpu.VMEM((2, dim, width), bf16),
            pltpu.VMEM((batch, width), bf16),
            pltpu.VMEM((batch, LANES), f32),
            pltpu.VMEM((blocks, dim, ROWS), f32),
            pltpu.VMEM((blocks, dim, ROWS), f32),
            pltpu.VMEM((batch, dim), f32),
            pltpu.VMEM((batch, dim), f32),
            pltpu.SemaphoreType.DMA((6,)),
            pltpu.SemaphoreType.DMA((2, 5)),
            pltpu.SemaphoreType.DMA((SLOTS, CHUNKS)),
            pltpu.SemaphoreType.DMA((SLOTS, CHUNKS)),
        ],
        compiler_params=pltpu.CompilerParams(vmem_limit_bytes=36 << 20),
        cost_estimate=pl.CostEstimate(flops=2 * batch * width * heads * dim * 5, transcendentals=0,
                                      bytes_accessed=2 * lin_state.size * 4 + 10 * heads * dim * width),
        name="lightning",
    )(in_hbm(slopes), in_hbm(cache_len), in_hbm(freq), in_hbm(norm_first.reshape(1, width)), in_hbm(out_norm), in_hbm(hidden), in_hbm(w_qkv.transpose(1, 2, 0, 3)),
      in_hbm(w_gate.transpose(1, 0, 2)), in_hbm(lin_state), in_hbm(w_out_lin))


def reduce_kernel(finish, chips, split, n_extra, part_ref, *refs):
    extra, (all_ref, own_ref), scratch = refs[:n_extra], refs[n_extra:n_extra + 2], refs[n_extra + 2:]
    pair_ref, acc_ref, up_a, up_b, up_c, down_a, down_b, down_c, gather_ref, send_sem, recv_sem = scratch
    width = part_ref.shape[2]
    out_width = gather_ref.shape[2]
    cut = out_width // 2
    me = lax.axis_index("tp")
    chip, core = me // 2, me % 2
    mate = 2 * chip + (1 - core)
    next_chip, prev_chip, far_chip = (chip + 1) % chips, (chip + chips - 1) % chips, (chip + 2) % chips
    up, down = 2 * next_chip + core, 2 * prev_chip + core

    barrier = pltpu.get_barrier_semaphore()
    for peer in (mate, up, down):
        pl.semaphore_signal(barrier, inc=1, device_id={"tp": peer}, device_id_type=MESH)
    pl.semaphore_wait(barrier, 3)

    counter = iter(range(64))

    def copy(src, dst, peer):
        i = next(counter)
        return pltpu.make_async_remote_copy(src_ref=src, dst_ref=dst, send_sem=send_sem.at[i], recv_sem=recv_sem.at[i],
                                            device_id={"tp": peer}, device_id_type=MESH)

    lo, hi = pl.ds(0, split), pl.ds(split, width - split)

    pair = [copy(part_ref.at[2 * t + (1 - core)], pair_ref.at[s], mate)
            for s, t in enumerate((far_chip, next_chip, prev_chip, chip))]
    for c in pair:
        c.start()
    pair[0].wait_recv()
    acc_ref[0] = part_ref[2 * far_chip + core] + pair_ref[0]
    far_up = copy(acc_ref.at[0, :, lo], up_a, up)
    far_down = copy(acc_ref.at[0, :, hi], down_a, down)
    far_up.start()
    far_down.start()
    pair[1].wait_recv()
    acc_ref[1] = part_ref[2 * next_chip + core] + pair_ref[1]
    near_up = copy(acc_ref.at[1, :, hi], up_b, up)
    near_up.start()
    pair[2].wait_recv()
    acc_ref[2] = part_ref[2 * prev_chip + core] + pair_ref[2]
    near_down = copy(acc_ref.at[2, :, lo], down_b, down)
    near_down.start()
    far_up.wait_recv()
    acc_ref[1, :, lo] += up_a[...]
    sum_up = copy(acc_ref.at[1, :, lo], up_c, up)
    sum_up.start()
    far_down.wait_recv()
    acc_ref[2, :, hi] += down_a[...]
    sum_down = copy(acc_ref.at[2, :, hi], down_c, down)
    sum_down.start()
    pair[3].wait_recv()
    acc_ref[3] = part_ref[me] + pair_ref[3]
    near_up.wait_recv()
    acc_ref[3, :, hi] += up_b[...]
    near_down.wait_recv()
    acc_ref[3, :, lo] += down_b[...]
    sum_up.wait_recv()
    acc_ref[3, :, lo] += up_c[...]
    sum_down.wait_recv()
    acc_ref[3, :, hi] += down_c[...]

    finish(me, acc_ref, own_ref, gather_ref, *extra)

    first, second = pl.ds(0, cut), pl.ds(cut, out_width - cut)

    def block(dev, cols):
        return gather_ref.at[dev, :, cols]

    def move(dev, cols, peer):
        return copy(block(dev, cols), block(dev, cols), peer)

    up_first, down_second = move(me, first, up), move(me, second, down)
    up_second, down_first = move(me, second, up), move(me, first, down)
    to_mate = move(me, pl.ds(0, out_width), mate)
    for c in (up_first, down_second, up_second, down_first, to_mate):
        c.start()
    sends = [to_mate]
    up_first.wait_recv()
    relay_up = move(down, first, up)
    relay_up.start()
    pass_0 = move(down, first, mate)
    pass_0.start()
    down_second.wait_recv()
    relay_down = move(up, second, down)
    relay_down.start()
    pass_1 = move(up, second, mate)
    pass_1.start()
    up_second.wait_recv()
    pass_2 = move(down, second, mate)
    pass_2.start()
    down_first.wait_recv()
    pass_3 = move(up, first, mate)
    pass_3.start()
    far = 2 * far_chip + core
    relay_up.wait_recv()
    pass_4 = move(far, first, mate)
    pass_4.start()
    relay_down.wait_recv()
    pass_5 = move(far, second, mate)
    pass_5.start()
    passes = [pass_0, pass_1, pass_2, pass_3, pass_4, pass_5]
    to_mate.wait_recv()
    for c in passes:
        c.wait_recv()
    all_ref[...] = gather_ref[...].reshape(all_ref.shape).astype(all_ref.dtype)
    for c in (pair + [far_up, far_down, near_up, near_down, sum_up, sum_down, up_first, down_second, up_second,
                      down_first, relay_up, relay_down] + sends + passes):
        c.wait_send()


def all_reduce(finish, collective_id, tp_size, part, extra, extra_specs, out_width, name):
    blocks, rows, width = part.shape
    split = (width // LANES + 1) // 2 * LANES
    chips = tp_size // 2
    f32 = jnp.float32
    return pl.pallas_call(
        functools.partial(reduce_kernel, finish, chips, split, len(extra)),
        out_shape=(jax.ShapeDtypeStruct((blocks * rows, out_width), jnp.bfloat16),
                   jax.ShapeDtypeStruct((rows, out_width), f32)),
        in_specs=[VMEM] + extra_specs,
        out_specs=(VMEM, VMEM),
        scratch_shapes=[
            pltpu.VMEM((chips, rows, width), f32),
            pltpu.VMEM((chips, rows, width), f32),
            pltpu.VMEM((rows, split), f32), pltpu.VMEM((rows, width - split), f32), pltpu.VMEM((rows, split), f32),
            pltpu.VMEM((rows, width - split), f32), pltpu.VMEM((rows, split), f32), pltpu.VMEM((rows, width - split), f32),
            pltpu.VMEM((blocks, rows, out_width), f32),
            pltpu.SemaphoreType.DMA((32,)), pltpu.SemaphoreType.DMA((32,)),
        ],
        compiler_params=pltpu.CompilerParams(collective_id=collective_id, has_side_effects=True,
                                             vmem_limit_bytes=8 << 20),
        cost_estimate=pl.CostEstimate(flops=10 ** 11, transcendentals=0, bytes_accessed=10 ** 8),
        name=name,
    )(part, *extra)


def finish_first(full_width, me, acc_ref, own_ref, gather_ref, h1_ref, norm_ref, alpha_ref, beta_ref):
    width = own_ref.shape[1]
    inv = lax.rsqrt(acc_ref[3, :, pl.ds(width, 1)] / full_width + EPS)
    lin = acc_ref[3, :, pl.ds(0, width)] * inv
    mid = (alpha_ref[0] * h1_ref[me] + beta_ref[0] * lin).astype(jnp.bfloat16).astype(jnp.float32)
    h2 = mid * lax.rsqrt(jnp.mean(mid * mid, axis=-1, keepdims=True) + EPS) * norm_ref[...]
    h2 = h2.astype(jnp.bfloat16).astype(jnp.float32)
    own_ref[...] = h2
    gather_ref[me] = h2


def finish_second(me, acc_ref, own_ref, gather_ref, h2_ref, alpha_ref, beta_ref):
    out = (alpha_ref[1] * h2_ref[...] + beta_ref[1] * acc_ref[3]).astype(jnp.bfloat16).astype(jnp.float32)
    own_ref[...] = out
    gather_ref[me] = out


def attention_kernel(len_ref, h2_ref, table_ref, pos_ref, watt_ref, k_ref, v_ref, wout_ref,
                     k_out_hbm, v_out_hbm, part_ref, q_ref, kn_ref, vn_ref, att_ref, patch_ref, bulk_sem, patch_sem):
    batch, width = h2_ref.shape
    group = watt_ref.shape[0] - 2
    dim = watt_ref.shape[2]
    tmax = k_ref.shape[2]
    per = 8
    sub = 16
    blocks = batch // per

    def bulk(i, which):
        src, dst = ((k_ref, k_out_hbm), (v_ref, v_out_hbm))[which]
        rows = pl.ds(i * per, per)
        return pltpu.make_async_copy(src.at[rows], dst.at[rows], bulk_sem.at[i, which])

    def patch(b, which):
        dst = (k_out_hbm, v_out_hbm)[which]
        start = pl.multiple_of((len_ref[b] // sub) * sub, sub)
        return pltpu.make_async_copy(patch_ref.at[which, b], dst.at[b, 0, pl.ds(start, sub)], patch_sem.at[b, which])

    for i in range(blocks):
        for which in range(2):
            bulk(i, which).start()

    h2 = h2_ref[...]

    def turn(x):
        return (x * table_ref[0] + pltpu.roll(x, dim - dim // 4, 1) * table_ref[1] + pltpu.roll(x, dim // 4, 1) * table_ref[2])

    q_ref[...] = jnp.zeros_like(q_ref)
    for j in range(group):
        q_ref[:, j, :] = turn(jnp.dot(h2, watt_ref[j], preferred_element_type=jnp.float32))
    kn_ref[...] = turn(jnp.dot(h2, watt_ref[group], preferred_element_type=jnp.float32)).astype(jnp.bfloat16).astype(jnp.float32)
    vn_ref[...] = jnp.dot(h2, watt_ref[group + 1], preferred_element_type=jnp.float32).astype(jnp.bfloat16).astype(jnp.float32)

    rows16 = lax.broadcasted_iota(jnp.int32, (sub, dim), 0)
    flat = per * ROWS
    cols = lax.broadcasted_iota(jnp.int32, (flat, tmax), 1)
    scale = dim ** -0.5

    def spread(rows):
        return jnp.concatenate([jnp.broadcast_to(rows[r:r + 1, :], (ROWS, dim)) for r in range(per)], axis=0)

    def block(i, _):
        base = pl.multiple_of(i * per, per)
        news = [kn_ref[pl.ds(base, per), :], vn_ref[pl.ds(base, per), :]]
        for r in range(per):
            b = base + r
            pos = len_ref[b]
            start = pl.multiple_of((pos // sub) * sub, sub)
            for which, ref in ((0, k_ref), (1, v_ref)):
                old = ref[b, 0, pl.ds(start, sub), :].astype(jnp.float32)
                patch_ref[which, b] = jnp.where(rows16 == pos - start, news[which][r:r + 1, :], old).astype(jnp.bfloat16)
        q = q_ref[pl.ds(base, per)].reshape(flat, dim)
        q_bf = q.astype(jnp.bfloat16)
        s_new = jnp.sum(q_bf.astype(jnp.float32) * spread(news[0]), axis=1, keepdims=True)
        scores = [lax.dot_general(q_bf[r * ROWS:(r + 1) * ROWS], k_ref[base + r, 0], (((1,), (1,)), ((), ())),
                                  preferred_element_type=jnp.float32) for r in range(per)]
        s = jnp.concatenate(scores, axis=0)
        pos = pos_ref[pl.ds(base, per)].reshape(flat, LANES)
        pos = jnp.concatenate([pos] * (tmax // LANES), axis=1)
        at_pos = cols == pos
        s = jnp.where(at_pos, s_new, s) * scale
        s = jnp.where(cols <= pos, s, -jnp.inf)
        e = jnp.exp(s - jnp.max(s, axis=1, keepdims=True))
        p = (e * (1.0 / jnp.sum(e, axis=1, keepdims=True))).astype(jnp.bfloat16).astype(jnp.float32)
        p_new = jnp.sum(jnp.where(at_pos, p, 0.0), axis=1, keepdims=True)
        p_old = jnp.where(at_pos, 0.0, p).astype(jnp.bfloat16)
        outs = [jnp.dot(p_old[r * ROWS:(r + 1) * ROWS], v_ref[base + r, 0], preferred_element_type=jnp.float32)
                for r in range(per)]
        att = jnp.concatenate(outs, axis=0) + p_new * spread(news[1])
        att_ref[pl.ds(base, per)] = att.reshape(per, ROWS, dim)
        for which in range(2):
            bulk(i, which).wait()
        for r in range(per):
            for which in range(2):
                patch(base + r, which).start()
        return 0

    lax.fori_loop(0, blocks, block, 0)
    rows = jnp.concatenate([att_ref[:, j, :] for j in range(group)], axis=1).astype(jnp.bfloat16)
    tile = 1024
    for c in range(width // tile):
        cs = pl.ds(c * tile, tile)
        piece = jnp.dot(rows, wout_ref[:, cs], preferred_element_type=jnp.float32)
        part_ref[:, :, cs] = piece.reshape(batch // ROWS, ROWS, tile)

    def finish(b, _):
        for which in range(2):
            patch(b, which).wait()
        return 0

    lax.fori_loop(0, batch, finish, 0)


def attention(cache_len, h2, w_attn, tables, positions, k_cache, v_cache, w_out):
    batch, width = h2.shape
    _, _, tmax, dim = k_cache.shape
    slots = w_attn.shape[0]
    blocks = batch // ROWS
    return pl.pallas_call(
        attention_kernel,
        out_shape=(pltpu.HBM(k_cache.shape, k_cache.dtype), pltpu.HBM(v_cache.shape, v_cache.dtype),
                   pltpu.VMEM((blocks, ROWS, width), jnp.float32)),
        in_specs=[SMEM] + [VMEM] * 7,
        out_specs=(HBM, HBM, VMEM),
        scratch_shapes=[
            pltpu.VMEM((batch, ROWS, dim), jnp.float32),
            pltpu.VMEM((batch, dim), jnp.float32),
            pltpu.VMEM((batch, dim), jnp.float32),
            pltpu.VMEM((batch, ROWS, dim), jnp.float32),
            pltpu.VMEM((2, batch, 16, dim), k_cache.dtype),
            pltpu.SemaphoreType.DMA((batch // 8, 2)),
            pltpu.SemaphoreType.DMA((batch, 2)),
        ],
        compiler_params=pltpu.CompilerParams(vmem_limit_bytes=8 << 20),
        cost_estimate=pl.CostEstimate(flops=2 * batch * width * dim * slots * 2, transcendentals=0,
                                      bytes_accessed=4 * k_cache.size * 2),
        name="attention",
    )(cache_len, h2, tables, positions, in_vmem(w_attn), in_vmem(k_cache), in_vmem(v_cache), in_vmem(w_out))


def rotary_freq(dim):
    rot = dim // 2
    half = rot // 2
    freq = ROPE_BASE ** (-2.0 * np.arange(half) / rot)
    return jnp.asarray(np.concatenate([freq, freq, np.zeros(dim - rot)])[None, :], jnp.float32)


def solution(mesh):
    tp_size = mesh.shape['tp']
    row_spec = P('dp', None)
    cache_spec = P('dp', 'tp', None, None)
    in_specs = (row_spec, P('dp'), cache_spec, cache_spec, cache_spec, P(None), P(None, None, 'tp', None),
                P(None, 'tp', None), P('tp'), P('tp', None), P('tp', None, None), P(None),
                P(None, 'tp', None, None), P('tp', None, None), P(None), P(None))
    out_specs = (row_spec, cache_spec, cache_spec, cache_spec)

    def local_step(hidden, cache_len, lin_state, k_cache, v_cache, norm_first, w_qkv, w_gate, slopes, out_norm,
                   w_out_lin, norm_second, w_attn, w_out_attn, mix_alpha, mix_beta):
        width = hidden.shape[1]
        dim = k_cache.shape[3]
        full_width = w_out_lin.shape[0] * dim * tp_size
        state_out, part, h1, tables, positions = lightning(hidden, cache_len, rotary_freq(dim), norm_first, w_qkv, w_gate, lin_state, slopes,
                                                out_norm, w_out_lin)
        h2, h2_own = all_reduce(functools.partial(finish_first, full_width), 0, tp_size, part,
                                (h1, norm_second.reshape(1, width), mix_alpha, mix_beta), [VMEM, VMEM, SMEM, SMEM],
                                width, "reduce_first")
        w_heads = w_attn.transpose(1, 2, 0, 3).reshape(w_attn.shape[2], width, dim)
        k_out, v_out, part = attention(cache_len, h2, w_heads, tables, positions, k_cache, v_cache,
                                       w_out_attn.reshape(w_out_attn.shape[0] * dim, width))
        hidden_out, _ = all_reduce(finish_second, 1, tp_size, part, (h2_own, mix_alpha, mix_beta), [VMEM, SMEM, SMEM],
                                   width, "reduce_second")
        return hidden_out, state_out, k_out, v_out

    return jax.shard_map(local_step, mesh=mesh, in_specs=in_specs, out_specs=out_specs, check_vma=False)
```

```python
import functools

import jax
import jax.numpy as jnp
import numpy as np
from jax import lax
from jax.experimental import pallas as pl
from jax.experimental.pallas import tpu as pltpu
from jax.sharding import PartitionSpec as P

EPS = 1e-5
ROPE_BASE = 10000000.0
MESH = pl.DeviceIdType.MESH
VMEM = pl.BlockSpec(memory_space=pltpu.VMEM)
SMEM = pl.BlockSpec(memory_space=pltpu.SMEM)
HBM = pl.BlockSpec(memory_space=pltpu.HBM)
ROWS = 8
LANES = 128
VMEM_LIMIT = 155 << 16


class Ring:
    def __init__(self, chips, send_sem, recv_sem):
        me = lax.axis_index("tp")
        self.me, chip, self.core = me, me // 2, me % 2
        self.order = ((chip + 2) % chips, (chip + 1) % chips, (chip + chips - 1) % chips, chip)
        self.mate = 2 * chip + (1 - self.core)
        self.up, self.down = 2 * self.order[1] + self.core, 2 * self.order[2] + self.core
        self.send_sem, self.recv_sem = send_sem, recv_sem
        self.copies = []

    def signal(self):
        for peer in (self.mate, self.up, self.down):
            pl.semaphore_signal(pltpu.get_barrier_semaphore(), inc=1, device_id={"tp": peer}, device_id_type=MESH)

    def wait(self):
        pl.semaphore_wait(pltpu.get_barrier_semaphore(), 3)

    def send(self, src, dst, peer):
        i = len(self.copies)
        c = pltpu.make_async_remote_copy(src_ref=src, dst_ref=dst, send_sem=self.send_sem.at[i], recv_sem=self.recv_sem.at[i],
                                         device_id={"tp": peer}, device_id_type=MESH)
        c.start()
        self.copies.append(c)
        return c

    def drain(self):
        for c in self.copies:
            c.wait_send()


class RowSum:
    def __init__(self, ring, split, part_ref, pair_ref, acc_ref, landing):
        self.ring, self.part, self.pair, self.acc, self.landing = ring, part_ref, pair_ref, acc_ref, landing
        width = part_ref.shape[2]
        self.lo, self.hi = pl.ds(0, split), pl.ds(split, width - split)
        self.mates = []

    def to_mate(self, s):
        t = self.ring.order[s]
        self.mates.append(self.ring.send(self.part.at[2 * t + (1 - self.ring.core)], self.pair.at[s], self.ring.mate))

    def add_mate(self, s):
        self.mates[s].wait_recv()
        self.acc[s] = self.part[2 * self.ring.order[s] + self.ring.core] + self.pair[s]

    def far(self):
        self.add_mate(0)
        self.far_up = self.ring.send(self.acc.at[0, :, self.lo], self.landing[0], self.ring.up)
        self.far_down = self.ring.send(self.acc.at[0, :, self.hi], self.landing[1], self.ring.down)

    def next(self):
        self.add_mate(1)
        self.near_up = self.ring.send(self.acc.at[1, :, self.hi], self.landing[2], self.ring.up)

    def previous(self):
        self.add_mate(2)
        self.near_down = self.ring.send(self.acc.at[2, :, self.lo], self.landing[3], self.ring.down)

    def relay(self):
        self.far_up.wait_recv()
        self.acc[1, :, self.lo] += self.landing[0][...]
        self.sum_up = self.ring.send(self.acc.at[1, :, self.lo], self.landing[4], self.ring.up)
        self.far_down.wait_recv()
        self.acc[2, :, self.hi] += self.landing[1][...]
        self.sum_down = self.ring.send(self.acc.at[2, :, self.hi], self.landing[5], self.ring.down)

    def own(self):
        self.add_mate(3)
        self.near_up.wait_recv()
        self.acc[3, :, self.hi] += self.landing[2][...]
        self.near_down.wait_recv()
        self.acc[3, :, self.lo] += self.landing[3][...]
        self.sum_up.wait_recv()
        self.acc[3, :, self.lo] += self.landing[4][...]
        self.sum_down.wait_recv()
        self.acc[3, :, self.hi] += self.landing[5][...]

    @staticmethod
    def scratch(chips, rows, width, split):
        f32 = jnp.float32
        halves = [pltpu.VMEM((rows, n), f32) for n in (split, width - split, width - split, split, split, width - split)]
        return [pltpu.VMEM((chips, rows, width), f32), pltpu.VMEM((chips, rows, width), f32)] + halves


def gather_rows(ring, gather_ref):
    out_width = gather_ref.shape[2]
    cut = out_width // 2
    first, second = pl.ds(0, cut), pl.ds(cut, out_width - cut)
    me, up, down, mate = ring.me, ring.up, ring.down, ring.mate
    far = 2 * ring.order[0] + ring.core

    def move(dev, cols, peer):
        return ring.send(gather_ref.at[dev, :, cols], gather_ref.at[dev, :, cols], peer)

    up_first, down_second = move(me, first, up), move(me, second, down)
    up_second, down_first = move(me, second, up), move(me, first, down)
    arrivals = [move(me, pl.ds(0, out_width), mate)]
    up_first.wait_recv()
    relay_up = move(down, first, up)
    arrivals.append(move(down, first, mate))
    down_second.wait_recv()
    relay_down = move(up, second, down)
    arrivals.append(move(up, second, mate))
    up_second.wait_recv()
    arrivals.append(move(down, second, mate))
    down_first.wait_recv()
    arrivals.append(move(up, first, mate))
    relay_up.wait_recv()
    arrivals.append(move(far, first, mate))
    relay_down.wait_recv()
    arrivals.append(move(far, second, mate))
    for c in arrivals:
        c.wait_recv()


def half_of(width):
    return (width // LANES + 1) // 2 * LANES


def second_kernel(chips, part_ref, h2_ref, alpha_ref, beta_ref, out_ref, pair_ref, acc_ref, *refs):
    landing, (gather_ref, send_sem, recv_sem) = refs[:6], refs[6:]
    ring = Ring(chips, send_sem, recv_sem)
    total = RowSum(ring, half_of(part_ref.shape[2]), part_ref, pair_ref, acc_ref, landing)
    ring.signal()
    ring.wait()
    for s in range(4):
        total.to_mate(s)
    total.far()
    total.next()
    total.previous()
    total.relay()
    total.own()
    out = alpha_ref[1] * h2_ref[...] + beta_ref[1] * acc_ref[3]
    gather_ref[ring.me] = out.astype(jnp.bfloat16).astype(jnp.float32)
    gather_rows(ring, gather_ref)
    out_ref[...] = gather_ref[...].reshape(out_ref.shape).astype(out_ref.dtype)
    ring.drain()


def second_sum(tp_size, part, h2_own, mix_alpha, mix_beta):
    blocks, rows, width = part.shape
    chips = tp_size // 2
    return pl.pallas_call(
        functools.partial(second_kernel, chips),
        out_shape=jax.ShapeDtypeStruct((blocks * rows, width), jnp.bfloat16),
        in_specs=[VMEM, VMEM, SMEM, SMEM],
        out_specs=VMEM,
        scratch_shapes=RowSum.scratch(chips, rows, width, half_of(width)) + [
            pltpu.VMEM((blocks, rows, width), jnp.float32),
            pltpu.SemaphoreType.DMA((32,)), pltpu.SemaphoreType.DMA((32,)),
        ],
        compiler_params=pltpu.CompilerParams(collective_id=1, has_side_effects=True, vmem_limit_bytes=VMEM_LIMIT),
        cost_estimate=pl.CostEstimate(flops=10 ** 11, transcendentals=0, bytes_accessed=10 ** 8),
        name="second_sum",
    )(part, h2_own, mix_alpha, mix_beta)


def first_kernel(chips, full_width,
                 slopes_hbm, len_hbm, freq_hbm, norm_hbm, onorm_hbm, norm2_hbm, alpha_hbm, beta_hbm, hidden_hbm,
                 wqkv_hbm, wgate_hbm, state_hbm, wout_hbm, watt_hbm, wout2_hbm, k_hbm, v_hbm,
                 state_ref, watt_ref, wout_ref, k_ref, v_ref, h2_ref, own_ref, table_ref, pos_ref,
                 slopes_ref, len_ref, freq_ref, norm_ref, onorm_ref, norm2_ref, alpha_ref, beta_ref,
                 h1_ref, proj_ref, o_ref, part_ref, gather_ref, small_sem, w_sem, wout_sem, state_sem, late_sem, send_sem, recv_sem,
                 pair_ref, acc_ref, *landing):
    batch, width = h2_ref.shape
    heads, dim = onorm_ref.shape
    slots = watt_ref.shape[0]
    blocks = batch // ROWS
    ring = Ring(chips, send_sem, recv_sem)
    total = RowSum(ring, half_of(part_ref.shape[2]), part_ref, pair_ref, acc_ref, landing)

    def piece(h, j):
        slot = (4 * h + j) % slots
        src = wqkv_hbm.at[j, h] if j < 3 else wgate_hbm.at[h]
        return pltpu.make_async_copy(src, watt_ref.at[slot], w_sem.at[slot])

    def wout_copy(h):
        return pltpu.make_async_copy(wout_hbm.at[h], wout_ref.at[h], wout_sem.at[h])

    def state_copy(s, half):
        rows = pl.ds(2 * ROWS * ring.order[s] + half * ROWS, ROWS)
        return pltpu.make_async_copy(state_hbm.at[rows], state_ref.at[rows], state_sem.at[s, half])

    small = [pltpu.make_async_copy(src, dst, small_sem.at[i])
             for i, (src, dst) in enumerate(((len_hbm, len_ref), (freq_hbm, freq_ref), (hidden_hbm, h2_ref), (norm_hbm, norm_ref),
                                             (slopes_hbm, slopes_ref), (onorm_hbm, onorm_ref), (norm2_hbm, norm2_ref),
                                             (alpha_hbm, alpha_ref), (beta_hbm, beta_ref)))]
    for c in small:
        c.start()
    for n in range(slots):
        piece(n // 4, n % 4).start()
    for c in small[:2]:
        c.wait()
    for r in range(batch):
        pos_ref[r] = jnp.full((ROWS, LANES), len_ref[r], jnp.int32)
    angle = pos_ref[:, 0, :].astype(jnp.float32) * freq_ref[...]
    cosine, sine = jnp.cos(angle), jnp.sin(angle)
    lane = lax.broadcasted_iota(jnp.int32, angle.shape, 1)
    table_ref[0] = jnp.where(lane < dim // 2, cosine, 1.0)
    table_ref[1] = jnp.where(lane < dim // 4, -sine, 0.0)
    table_ref[2] = jnp.where((lane >= dim // 4) & (lane < dim // 2), sine, 0.0)

    for c in small[2:]:
        c.wait()
    x = h2_ref[...].astype(jnp.float32)
    h1 = x * lax.rsqrt(jnp.mean(x * x, axis=-1, keepdims=True) + EPS) * norm_ref[...]
    h1 = h1.astype(jnp.bfloat16)
    h1_ref[...] = h1
    gather_ref[...] = h1.astype(jnp.float32).reshape(gather_ref.shape)
    ring.signal()

    def one_head(h, _):
        for j in range(4):
            piece(h, j).wait()
            y = jnp.dot(h1_ref[...], watt_ref[(4 * h + j) % slots], preferred_element_type=jnp.float32)
            gate = jax.nn.sigmoid(y)
            proj_ref[j, h] = gate if j == 3 else (y * gate).astype(jnp.bfloat16).astype(jnp.float32)
            ahead, later = (j + slots) // 4, (j + slots) % 4

            @pl.when(h + ahead < heads)
            def _():
                piece(h + ahead, later).start()

            @pl.when(h == heads - 2)
            def _():
                if j == 1:
                    for i in range(heads // 2):
                        wout_copy(i).start()
                if j >= 2:
                    state_copy(0, j - 2).start()

            @pl.when(h == heads - 1)
            def _():
                if j == 0:
                    for i in range(heads // 2, heads):
                        wout_copy(i).start()
                if j >= 2:
                    state_copy(1, j - 2).start()
        return 0

    lax.fori_loop(0, heads, one_head, 0)
    ring.wait()

    late = [pltpu.make_async_copy(watt_hbm.at[j], watt_ref.at[j], late_sem.at[0, j]) for j in range(slots)]
    caches = [pltpu.make_async_copy(src.at[pl.ds(i * 16, 16)], dst.at[pl.ds(i * 16, 16)], late_sem.at[1 + which, i])
              for which, (src, dst) in enumerate(((k_hbm, k_ref), (v_hbm, v_ref))) for i in range(batch // 16)]
    wout2 = [pltpu.make_async_copy(wout2_hbm.at[h], wout_ref.at[h], late_sem.at[3, h]) for h in range(heads)]

    pair_rows = 2 * ROWS
    wide = ROWS * dim
    row_id = lax.broadcasted_iota(jnp.int32, (pair_rows, wide), 0)
    lane_block = lax.broadcasted_iota(jnp.int32, (pair_rows, wide), 1) // dim
    contract = (((0,), (0,)), ((), ()))

    def update(base):
        def body(h, _):
            decay = jnp.exp(-jnp.full((1, dim), slopes_ref[h], jnp.float32))
            rows = pl.ds(base, pair_rows)
            q = proj_ref[0, h, rows, :].astype(jnp.bfloat16)
            k = proj_ref[1, h, rows, :].astype(jnp.bfloat16)
            v = jnp.concatenate([proj_ref[2, h, rows, :]] * ROWS, axis=1)
            for half in range(2):
                mine = lane_block + half * ROWS == row_id
                spread_v = jnp.where(mine, v, 0.0).astype(jnp.bfloat16)
                ones = jnp.where(mine, 1.0, 0.0).astype(jnp.bfloat16)
                outer = lax.dot_general(k, spread_v, contract, preferred_element_type=jnp.float32)
                q_all = lax.dot_general(q, ones, contract, preferred_element_type=jnp.float32)
                outs = []
                for r in range(ROWS):
                    row = base + half * ROWS + r
                    cols = slice(r * dim, (r + 1) * dim)
                    new = decay * state_ref[row, h] + outer[:, cols]
                    state_ref[row, h] = new
                    outs.append(jnp.sum(q_all[:, cols] * new, axis=0, keepdims=True))
                o_ref[h, pl.ds(half * ROWS, ROWS), :] = jnp.concatenate(outs, axis=0)
            return 0

        lax.fori_loop(0, heads, body, 0)

    def project_out(t, base):
        squares = jnp.zeros((pair_rows, 1), jnp.float32)
        gated = []
        for h in range(heads):
            o = o_ref[h]
            squares += jnp.sum(o * o, axis=1, keepdims=True)
            gated.append((o * onorm_ref[h:h + 1, :] * proj_ref[3, h, pl.ds(base, pair_rows), :]).astype(jnp.bfloat16))
        gated = jnp.concatenate(gated, axis=1)
        tile = 1024
        for c in range(width // tile):
            cols = pl.ds(c * tile, tile)
            w = wout_ref[:, :, cols].reshape(heads * dim, tile)
            y = jnp.dot(gated, w, preferred_element_type=jnp.float32)
            part_ref[pl.ds(2 * t, 2), :, cols] = y.reshape(2, ROWS, tile)
        part_ref[pl.ds(2 * t, 2), :, pl.ds(width, LANES)] = jnp.broadcast_to(squares, (pair_rows, LANES)).reshape(2, ROWS, LANES)

    for s in range(4):
        t = ring.order[s]
        base = pl.multiple_of(t * pair_rows, pair_rows)
        for c in [state_copy(s + 2, 0), state_copy(s + 2, 1)] if s < 2 else (late, caches)[s - 2]:
            c.start()
        for half in range(2):
            state_copy(s, half).wait()
        update(base)
        if s == 0:
            for h in range(heads):
                wout_copy(h).wait()
        if s == 3:
            total.previous()
            total.relay()
        project_out(t, base)
        total.to_mate(s)
        if s == 1:
            total.far()
        if s == 2:
            total.next()
    for c in wout2:
        c.start()
    total.own()

    inv = lax.rsqrt(acc_ref[3, :, pl.ds(width, 1)] / full_width + EPS)
    lin = acc_ref[3, :, pl.ds(0, width)] * inv
    mid = (alpha_ref[0] * gather_ref[ring.me] + beta_ref[0] * lin).astype(jnp.bfloat16).astype(jnp.float32)
    h2 = mid * lax.rsqrt(jnp.mean(mid * mid, axis=-1, keepdims=True) + EPS) * norm2_ref[...]
    h2 = h2.astype(jnp.bfloat16).astype(jnp.float32)
    own_ref[...] = h2
    gather_ref[ring.me] = h2
    gather_rows(ring, gather_ref)
    h2_ref[...] = gather_ref[...].reshape(h2_ref.shape).astype(h2_ref.dtype)
    ring.drain()
    for c in late + caches + wout2:
        c.wait()


def in_hbm(x):
    return pltpu.with_memory_space_constraint(x, pltpu.HBM)


def in_vmem(x):
    return pltpu.with_memory_space_constraint(x, pltpu.VMEM)


def first_sublayer(tp_size, slopes, cache_len, freq, norm_first, out_norm, norm_second, mix_alpha, mix_beta, hidden,
                   w_qkv, w_gate, lin_state, w_out_lin, w_attn, w_out_attn, k_cache, v_cache):
    batch, width = hidden.shape
    heads, dim = out_norm.shape
    blocks = batch // ROWS
    slots = w_attn.shape[0]
    chips = tp_size // 2
    f32, bf16 = jnp.float32, jnp.bfloat16
    part_width = width + LANES
    args = (slopes, cache_len, freq, norm_first.reshape(1, width), out_norm, norm_second.reshape(1, width), mix_alpha, mix_beta, hidden,
            w_qkv, w_gate, lin_state, w_out_lin, w_attn, w_out_attn, k_cache, v_cache)
    dma = pltpu.SemaphoreType.DMA
    return pl.pallas_call(
        functools.partial(first_kernel, chips, heads * dim * tp_size),
        out_shape=(pltpu.VMEM(lin_state.shape, f32),
                   pltpu.VMEM((slots, width, dim), bf16),
                   pltpu.VMEM((heads, dim, width), bf16),
                   pltpu.VMEM(k_cache.shape, k_cache.dtype),
                   pltpu.VMEM(v_cache.shape, v_cache.dtype),
                   pltpu.VMEM((batch, width), bf16),
                   pltpu.VMEM((ROWS, width), f32),
                   pltpu.VMEM((3, batch, dim), f32),
                   pltpu.VMEM((batch, ROWS, LANES), jnp.int32)),
        in_specs=[HBM] * len(args),
        out_specs=(VMEM,) * 9,
        scratch_shapes=[
            pltpu.SMEM((heads,), f32), pltpu.SMEM((batch,), jnp.int32), pltpu.VMEM((1, dim), f32), pltpu.VMEM((1, width), f32),
            pltpu.VMEM((heads, dim), f32), pltpu.VMEM((1, width), f32), pltpu.SMEM((2,), f32), pltpu.SMEM((2,), f32),
            pltpu.VMEM((batch, width), bf16),
            pltpu.VMEM((4, heads, batch, dim), f32),
            pltpu.VMEM((heads, 2 * ROWS, dim), f32),
            pltpu.VMEM((blocks, ROWS, part_width), f32),
            pltpu.VMEM((blocks, ROWS, width), f32),
            dma((9,)), dma((slots,)), dma((heads,)), dma((4, 2)), dma((4, 8)), dma((32,)), dma((32,)),
        ] + RowSum.scratch(chips, ROWS, part_width, half_of(part_width)),
        compiler_params=pltpu.CompilerParams(collective_id=0, has_side_effects=True, vmem_limit_bytes=VMEM_LIMIT),
        cost_estimate=pl.CostEstimate(flops=10 ** 11, transcendentals=0, bytes_accessed=10 ** 8),
        name="first_sublayer",
    )(*[in_hbm(x) for x in args])


def attention_kernel(len_ref, h2_ref, table_ref, pos_ref, watt_ref, k_ref, v_ref, wout_ref, state_ref,
                     k_out_hbm, v_out_hbm, state_out_hbm, part_ref, q_ref, kn_ref, vn_ref, att_ref, patch_ref, bulk_sem, patch_sem,
                     state_sem):
    batch, width = h2_ref.shape
    group = watt_ref.shape[0] - 2
    dim = watt_ref.shape[2]
    tmax = k_ref.shape[2]
    per = 8
    sub = 16
    blocks = batch // per

    def bulk(i, which):
        src, dst = ((k_ref, k_out_hbm), (v_ref, v_out_hbm))[which]
        rows = pl.ds(i * per, per)
        return pltpu.make_async_copy(src.at[rows], dst.at[rows], bulk_sem.at[i, which])

    def patch(b, which):
        dst = (k_out_hbm, v_out_hbm)[which]
        start = pl.multiple_of((len_ref[b] // sub) * sub, sub)
        return pltpu.make_async_copy(patch_ref.at[which, b], dst.at[b, 0, pl.ds(start, sub)], patch_sem.at[b, which])

    for i in range(blocks):
        for which in range(2):
            bulk(i, which).start()
    states = [pltpu.make_async_copy(state_ref.at[pl.ds(i * per, per)], state_out_hbm.at[pl.ds(i * per, per)], state_sem.at[i])
              for i in range(blocks)]
    for c in states:
        c.start()

    h2 = h2_ref[...]

    def turn(x):
        return (x * table_ref[0] + pltpu.roll(x, dim - dim // 4, 1) * table_ref[1] + pltpu.roll(x, dim // 4, 1) * table_ref[2])

    q_ref[...] = jnp.zeros_like(q_ref)
    for j in range(group):
        q_ref[:, j, :] = turn(jnp.dot(h2, watt_ref[j], preferred_element_type=jnp.float32))
    kn_ref[...] = turn(jnp.dot(h2, watt_ref[group], preferred_element_type=jnp.float32)).astype(jnp.bfloat16).astype(jnp.float32)
    vn_ref[...] = jnp.dot(h2, watt_ref[group + 1], preferred_element_type=jnp.float32).astype(jnp.bfloat16).astype(jnp.float32)

    rows16 = lax.broadcasted_iota(jnp.int32, (sub, dim), 0)
    flat = per * ROWS
    cols = lax.broadcasted_iota(jnp.int32, (flat, tmax), 1)
    scale = dim ** -0.5

    def spread(rows):
        return jnp.concatenate([jnp.broadcast_to(rows[r:r + 1, :], (ROWS, dim)) for r in range(per)], axis=0)

    def block(i, _):
        base = pl.multiple_of(i * per, per)
        news = [kn_ref[pl.ds(base, per), :], vn_ref[pl.ds(base, per), :]]
        for r in range(per):
            b = base + r
            pos = len_ref[b]
            start = pl.multiple_of((pos // sub) * sub, sub)
            for which, ref in ((0, k_ref), (1, v_ref)):
                old = ref[b, 0, pl.ds(start, sub), :].astype(jnp.float32)
                patch_ref[which, b] = jnp.where(rows16 == pos - start, news[which][r:r + 1, :], old).astype(jnp.bfloat16)
        q = q_ref[pl.ds(base, per)].reshape(flat, dim)
        q_bf = q.astype(jnp.bfloat16)
        s_new = jnp.sum(q_bf.astype(jnp.float32) * spread(news[0]), axis=1, keepdims=True)
        scores = [lax.dot_general(q_bf[r * ROWS:(r + 1) * ROWS], k_ref[base + r, 0], (((1,), (1,)), ((), ())),
                                  preferred_element_type=jnp.float32) for r in range(per)]
        s = jnp.concatenate(scores, axis=0)
        pos = pos_ref[pl.ds(base, per)].reshape(flat, LANES)
        pos = jnp.concatenate([pos] * (tmax // LANES), axis=1)
        at_pos = cols == pos
        s = jnp.where(at_pos, s_new, s) * scale
        s = jnp.where(cols <= pos, s, -jnp.inf)
        e = jnp.exp(s - jnp.max(s, axis=1, keepdims=True))
        p = (e * (1.0 / jnp.sum(e, axis=1, keepdims=True))).astype(jnp.bfloat16).astype(jnp.float32)
        p_new = jnp.sum(jnp.where(at_pos, p, 0.0), axis=1, keepdims=True)
        p_old = jnp.where(at_pos, 0.0, p).astype(jnp.bfloat16)
        outs = [jnp.dot(p_old[r * ROWS:(r + 1) * ROWS], v_ref[base + r, 0], preferred_element_type=jnp.float32)
                for r in range(per)]
        att = jnp.concatenate(outs, axis=0) + p_new * spread(news[1])
        att_ref[pl.ds(base, per)] = att.reshape(per, ROWS, dim)
        for which in range(2):
            bulk(i, which).wait()
        for r in range(per):
            for which in range(2):
                patch(base + r, which).start()
        return 0

    lax.fori_loop(0, blocks, block, 0)
    rows = jnp.concatenate([att_ref[:, j, :] for j in range(group)], axis=1).astype(jnp.bfloat16)
    tile = 1024
    for c in range(width // tile):
        cs = pl.ds(c * tile, tile)
        piece = jnp.dot(rows, wout_ref[:, :, cs].reshape(group * dim, tile), preferred_element_type=jnp.float32)
        part_ref[:, :, cs] = piece.reshape(batch // ROWS, ROWS, tile)

    def finish(b, _):
        for which in range(2):
            patch(b, which).wait()
        return 0

    lax.fori_loop(0, batch, finish, 0)
    for c in states:
        c.wait()


def attention(cache_len, h2, w_attn, tables, positions, k_cache, v_cache, w_out, state):
    batch, width = h2.shape
    _, _, tmax, dim = k_cache.shape
    slots = w_attn.shape[0]
    blocks = batch // ROWS
    return pl.pallas_call(
        attention_kernel,
        out_shape=(pltpu.HBM(k_cache.shape, k_cache.dtype), pltpu.HBM(v_cache.shape, v_cache.dtype),
                   pltpu.HBM(state.shape, state.dtype),
                   pltpu.VMEM((blocks, ROWS, width), jnp.float32)),
        in_specs=[SMEM] + [VMEM] * 8,
        out_specs=(HBM, HBM, HBM, VMEM),
        scratch_shapes=[
            pltpu.VMEM((batch, ROWS, dim), jnp.float32),
            pltpu.VMEM((batch, dim), jnp.float32),
            pltpu.VMEM((batch, dim), jnp.float32),
            pltpu.VMEM((batch, ROWS, dim), jnp.float32),
            pltpu.VMEM((2, batch, 16, dim), k_cache.dtype),
            pltpu.SemaphoreType.DMA((batch // 8, 2)),
            pltpu.SemaphoreType.DMA((batch, 2)),
            pltpu.SemaphoreType.DMA((batch // 8,)),
        ],
        compiler_params=pltpu.CompilerParams(vmem_limit_bytes=VMEM_LIMIT),
        cost_estimate=pl.CostEstimate(flops=2 * batch * width * dim * slots * 2, transcendentals=0,
                                      bytes_accessed=4 * k_cache.size * 2),
        name="attention",
    )(cache_len, *[in_vmem(x) for x in (h2, tables, positions, w_attn, k_cache, v_cache, w_out, state)])


def rotary_freq(dim):
    rot = dim // 2
    half = rot // 2
    freq = ROPE_BASE ** (-2.0 * np.arange(half) / rot)
    return jnp.asarray(np.concatenate([freq, freq, np.zeros(dim - rot)])[None, :], jnp.float32)


def solution(mesh):
    tp_size = mesh.shape['tp']
    row_spec = P('dp', None)
    cache_spec = P('dp', 'tp', None, None)
    in_specs = (row_spec, P('dp'), cache_spec, cache_spec, cache_spec, P(None), P(None, None, 'tp', None),
                P(None, 'tp', None), P('tp'), P('tp', None), P('tp', None, None), P(None),
                P(None, 'tp', None, None), P('tp', None, None), P(None), P(None))
    out_specs = (row_spec, cache_spec, cache_spec, cache_spec)

    def local_step(hidden, cache_len, lin_state, k_cache, v_cache, norm_first, w_qkv, w_gate, slopes, out_norm,
                   w_out_lin, norm_second, w_attn, w_out_attn, mix_alpha, mix_beta):
        width = hidden.shape[1]
        dim = k_cache.shape[3]
        w_heads = w_attn.transpose(1, 2, 0, 3).reshape(w_attn.shape[2], width, dim)
        state, w_heads, w_out, keys, values, h2, h2_own, tables, positions = first_sublayer(
            tp_size, slopes, cache_len, rotary_freq(dim), norm_first, out_norm, norm_second, mix_alpha, mix_beta, hidden,
            w_qkv.transpose(1, 2, 0, 3), w_gate.transpose(1, 0, 2), lin_state, w_out_lin, w_heads, w_out_attn, k_cache, v_cache)
        k_out, v_out, state_out, part = attention(cache_len, h2, w_heads, tables, positions, keys, values, w_out, state)
        hidden_out = second_sum(tp_size, part, h2_own, mix_alpha, mix_beta)
        return hidden_out, state_out, k_out, v_out

    return jax.shard_map(local_step, mesh=mesh, in_specs=in_specs, out_specs=out_specs, check_vma=False)
```

```python
import functools

import jax
import jax.numpy as jnp
import numpy as np
from jax import lax
from jax.experimental import pallas as pl
from jax.experimental.pallas import tpu as pltpu
from jax.sharding import PartitionSpec as P

EPS = 1e-5
ROPE_BASE = 10000000.0
MESH = pl.DeviceIdType.MESH
VMEM = pl.BlockSpec(memory_space=pltpu.VMEM)
SMEM = pl.BlockSpec(memory_space=pltpu.SMEM)
HBM = pl.BlockSpec(memory_space=pltpu.HBM)
ROWS = 8
LANES = 128
VMEM_LIMIT = 155 << 16


class Ring:
    def __init__(self, chips, send_sem, recv_sem):
        me = lax.axis_index("tp")
        self.me, chip, self.core = me, me // 2, me % 2
        self.order = ((chip + 2) % chips, (chip + 1) % chips, (chip + chips - 1) % chips, chip)
        self.mate = 2 * chip + (1 - self.core)
        self.up, self.down = 2 * self.order[1] + self.core, 2 * self.order[2] + self.core
        self.send_sem, self.recv_sem = send_sem, recv_sem
        self.copies = []

    def signal(self):
        for peer in (self.mate, self.up, self.down):
            pl.semaphore_signal(pltpu.get_barrier_semaphore(), inc=1, device_id={"tp": peer}, device_id_type=MESH)

    def wait(self):
        pl.semaphore_wait(pltpu.get_barrier_semaphore(), 3)

    def send(self, src, dst, peer):
        i = len(self.copies)
        c = pltpu.make_async_remote_copy(src_ref=src, dst_ref=dst, send_sem=self.send_sem.at[i], recv_sem=self.recv_sem.at[i],
                                         device_id={"tp": peer}, device_id_type=MESH)
        c.start()
        self.copies.append(c)
        return c

    def drain(self):
        for c in self.copies:
            c.wait_send()


class RowSum:
    def __init__(self, ring, split, part_ref, pair_ref, acc_ref, landing):
        self.ring, self.part, self.pair, self.acc, self.landing = ring, part_ref, pair_ref, acc_ref, landing
        width = part_ref.shape[2]
        self.lo, self.hi = pl.ds(0, split), pl.ds(split, width - split)
        self.mates = []

    def to_mate(self, s):
        t = self.ring.order[s]
        self.mates.append(self.ring.send(self.part.at[2 * t + (1 - self.ring.core)], self.pair.at[s], self.ring.mate))

    def add_mate(self, s):
        self.mates[s].wait_recv()
        self.acc[s] = self.part[2 * self.ring.order[s] + self.ring.core] + self.pair[s]

    def far(self):
        self.add_mate(0)
        self.far_up = self.ring.send(self.acc.at[0, :, self.lo], self.landing[0], self.ring.up)
        self.far_down = self.ring.send(self.acc.at[0, :, self.hi], self.landing[1], self.ring.down)

    def next(self):
        self.add_mate(1)
        self.near_up = self.ring.send(self.acc.at[1, :, self.hi], self.landing[2], self.ring.up)

    def previous(self):
        self.add_mate(2)
        self.near_down = self.ring.send(self.acc.at[2, :, self.lo], self.landing[3], self.ring.down)

    def relay(self):
        self.far_up.wait_recv()
        self.acc[1, :, self.lo] += self.landing[0][...]
        self.sum_up = self.ring.send(self.acc.at[1, :, self.lo], self.landing[4], self.ring.up)
        self.far_down.wait_recv()
        self.acc[2, :, self.hi] += self.landing[1][...]
        self.sum_down = self.ring.send(self.acc.at[2, :, self.hi], self.landing[5], self.ring.down)

    def own(self):
        self.add_mate(3)
        self.near_up.wait_recv()
        self.acc[3, :, self.hi] += self.landing[2][...]
        self.near_down.wait_recv()
        self.acc[3, :, self.lo] += self.landing[3][...]
        self.sum_up.wait_recv()
        self.acc[3, :, self.lo] += self.landing[4][...]
        self.sum_down.wait_recv()
        self.acc[3, :, self.hi] += self.landing[5][...]

    @staticmethod
    def scratch(chips, rows, width, split):
        f32 = jnp.float32
        halves = [pltpu.VMEM((rows, n), f32) for n in (split, width - split, width - split, split, split, width - split)]
        return [pltpu.VMEM((chips, rows, width), f32), pltpu.VMEM((chips, rows, width), f32)] + halves


def gather_rows(ring, gather_ref):
    out_width = gather_ref.shape[2]
    cut = out_width // 2
    first, second = pl.ds(0, cut), pl.ds(cut, out_width - cut)
    me, up, down, mate = ring.me, ring.up, ring.down, ring.mate
    far = 2 * ring.order[0] + ring.core

    def move(dev, cols, peer):
        return ring.send(gather_ref.at[dev, :, cols], gather_ref.at[dev, :, cols], peer)

    up_first, down_second = move(me, first, up), move(me, second, down)
    up_second, down_first = move(me, second, up), move(me, first, down)
    arrivals = [move(me, pl.ds(0, out_width), mate)]
    up_first.wait_recv()
    relay_up = move(down, first, up)
    arrivals.append(move(down, first, mate))
    down_second.wait_recv()
    relay_down = move(up, second, down)
    arrivals.append(move(up, second, mate))
    up_second.wait_recv()
    arrivals.append(move(down, second, mate))
    down_first.wait_recv()
    arrivals.append(move(up, first, mate))
    relay_up.wait_recv()
    arrivals.append(move(far, first, mate))
    relay_down.wait_recv()
    arrivals.append(move(far, second, mate))
    for c in arrivals:
        c.wait_recv()


def half_of(width):
    return (width // LANES + 1) // 2 * LANES


def second_kernel(chips, part_ref, h2_ref, alpha_ref, beta_ref, out_ref, pair_ref, acc_ref, *refs):
    landing, (gather_ref, send_sem, recv_sem) = refs[:6], refs[6:]
    ring = Ring(chips, send_sem, recv_sem)
    total = RowSum(ring, half_of(part_ref.shape[2]), part_ref, pair_ref, acc_ref, landing)
    ring.signal()
    ring.wait()
    for s in range(4):
        total.to_mate(s)
    total.far()
    total.next()
    total.previous()
    total.relay()
    total.own()
    out = alpha_ref[1] * h2_ref[...] + beta_ref[1] * acc_ref[3]
    gather_ref[ring.me] = out.astype(jnp.bfloat16).astype(jnp.float32)
    gather_rows(ring, gather_ref)
    out_ref[...] = gather_ref[...].reshape(out_ref.shape).astype(out_ref.dtype)
    ring.drain()


def second_sum(tp_size, part, h2_own, mix_alpha, mix_beta):
    blocks, rows, width = part.shape
    chips = tp_size // 2
    return pl.pallas_call(
        functools.partial(second_kernel, chips),
        out_shape=jax.ShapeDtypeStruct((blocks * rows, width), jnp.bfloat16),
        in_specs=[VMEM, VMEM, SMEM, SMEM],
        out_specs=VMEM,
        scratch_shapes=RowSum.scratch(chips, rows, width, half_of(width)) + [
            pltpu.VMEM((blocks, rows, width), jnp.float32),
            pltpu.SemaphoreType.DMA((32,)), pltpu.SemaphoreType.DMA((32,)),
        ],
        compiler_params=pltpu.CompilerParams(collective_id=1, has_side_effects=True, vmem_limit_bytes=VMEM_LIMIT),
        cost_estimate=pl.CostEstimate(flops=10 ** 11, transcendentals=0, bytes_accessed=10 ** 8),
        name="second_sum",
    )(part, h2_own, mix_alpha, mix_beta)


def first_kernel(chips, full_width,
                 slopes_hbm, len_hbm, freq_hbm, norm_hbm, onorm_hbm, norm2_hbm, alpha_hbm, beta_hbm, hidden_hbm,
                 wqkv_hbm, wgate_hbm, state_hbm, wout_hbm, watt_hbm, wout2_hbm, k_hbm, v_hbm,
                 state_ref, watt_ref, wout_ref, k_ref, v_ref, h2_ref, own_ref, table_ref, pos_ref,
                 slopes_ref, len_ref, freq_ref, norm_ref, onorm_ref, norm2_ref, alpha_ref, beta_ref,
                 h1_ref, proj_ref, o_ref, part_ref, gather_ref, small_sem, w_sem, wout_sem, state_sem, late_sem, send_sem, recv_sem,
                 pair_ref, acc_ref, *landing):
    batch, width = h2_ref.shape
    heads, dim = onorm_ref.shape
    slots = watt_ref.shape[0]
    blocks = batch // ROWS
    ring = Ring(chips, send_sem, recv_sem)
    total = RowSum(ring, half_of(part_ref.shape[2]), part_ref, pair_ref, acc_ref, landing)

    def piece(h, j):
        slot = (4 * h + j) % slots
        src = wqkv_hbm.at[j, h] if j < 3 else wgate_hbm.at[h]
        return pltpu.make_async_copy(src, watt_ref.at[slot], w_sem.at[slot])

    def wout_copy(h):
        return pltpu.make_async_copy(wout_hbm.at[h], wout_ref.at[h], wout_sem.at[h])

    def state_copy(s, half):
        rows = pl.ds(2 * ROWS * ring.order[s] + half * ROWS, ROWS)
        return pltpu.make_async_copy(state_hbm.at[rows], state_ref.at[rows], state_sem.at[s, half])

    small = [pltpu.make_async_copy(src, dst, small_sem.at[i])
             for i, (src, dst) in enumerate(((len_hbm, len_ref), (freq_hbm, freq_ref), (hidden_hbm, h2_ref), (norm_hbm, norm_ref),
                                             (slopes_hbm, slopes_ref), (onorm_hbm, onorm_ref), (norm2_hbm, norm2_ref),
                                             (alpha_hbm, alpha_ref), (beta_hbm, beta_ref)))]
    for c in small:
        c.start()
    for n in range(slots):
        piece(n // 4, n % 4).start()
    for c in small[:2]:
        c.wait()
    for r in range(batch):
        pos_ref[r] = jnp.full((ROWS, LANES), len_ref[r], jnp.int32)
    angle = pos_ref[:, 0, :].astype(jnp.float32) * freq_ref[...]
    cosine, sine = jnp.cos(angle), jnp.sin(angle)
    lane = lax.broadcasted_iota(jnp.int32, angle.shape, 1)
    table_ref[0] = jnp.where(lane < dim // 2, cosine, 1.0)
    table_ref[1] = jnp.where(lane < dim // 4, -sine, 0.0)
    table_ref[2] = jnp.where((lane >= dim // 4) & (lane < dim // 2), sine, 0.0)

    for c in small[2:]:
        c.wait()
    x = h2_ref[...].astype(jnp.float32)
    h1 = x * lax.rsqrt(jnp.mean(x * x, axis=-1, keepdims=True) + EPS) * norm_ref[...]
    h1 = h1.astype(jnp.bfloat16)
    h1_ref[...] = h1
    gather_ref[...] = h1.astype(jnp.float32).reshape(gather_ref.shape)
    ring.signal()

    def one_head(h, _):
        for j in range(4):
            piece(h, j).wait()
            y = jnp.dot(h1_ref[...], watt_ref[(4 * h + j) % slots], preferred_element_type=jnp.float32)
            gate = jax.nn.sigmoid(y)
            proj_ref[j, h] = gate if j == 3 else (y * gate).astype(jnp.bfloat16).astype(jnp.float32)
            ahead, later = (j + slots) // 4, (j + slots) % 4

            @pl.when(h + ahead < heads)
            def _():
                piece(h + ahead, later).start()

            @pl.when(h == heads - 2)
            def _():
                if j == 1:
                    for i in range(heads // 2):
                        wout_copy(i).start()
                if j >= 2:
                    state_copy(0, j - 2).start()

            @pl.when(h == heads - 1)
            def _():
                if j == 0:
                    for i in range(heads // 2, heads):
                        wout_copy(i).start()
                if j >= 2:
                    state_copy(1, j - 2).start()
        return 0

    lax.fori_loop(0, heads, one_head, 0)
    ring.wait()

    late = [pltpu.make_async_copy(watt_hbm.at[j], watt_ref.at[j], late_sem.at[0, j]) for j in range(slots)]
    caches = [pltpu.make_async_copy(src.at[pl.ds(i * 16, 16)], dst.at[pl.ds(i * 16, 16)], late_sem.at[1 + which, i])
              for which, (src, dst) in enumerate(((k_hbm, k_ref), (v_hbm, v_ref))) for i in range(batch // 16)]
    wout2 = [pltpu.make_async_copy(wout2_hbm.at[h], wout_ref.at[h], late_sem.at[3, h]) for h in range(heads)]

    pair_rows = 2 * ROWS
    wide = ROWS * dim
    row_id = lax.broadcasted_iota(jnp.int32, (pair_rows, wide), 0)
    lane_block = lax.broadcasted_iota(jnp.int32, (pair_rows, wide), 1) // dim
    contract = (((0,), (0,)), ((), ()))

    def update(base):
        def body(h, _):
            decay = jnp.exp(-jnp.full((1, dim), slopes_ref[h], jnp.float32))
            rows = pl.ds(base, pair_rows)
            q = proj_ref[0, h, rows, :].astype(jnp.bfloat16)
            k = proj_ref[1, h, rows, :].astype(jnp.bfloat16)
            v = jnp.concatenate([proj_ref[2, h, rows, :]] * ROWS, axis=1)
            for half in range(2):
                mine = lane_block + half * ROWS == row_id
                spread_v = jnp.where(mine, v, 0.0).astype(jnp.bfloat16)
                ones = jnp.where(mine, 1.0, 0.0).astype(jnp.bfloat16)
                outer = lax.dot_general(k, spread_v, contract, preferred_element_type=jnp.float32)
                q_all = lax.dot_general(q, ones, contract, preferred_element_type=jnp.float32)
                outs = []
                for r in range(ROWS):
                    row = base + half * ROWS + r
                    cols = slice(r * dim, (r + 1) * dim)
                    new = decay * state_ref[row, h] + outer[:, cols]
                    state_ref[row, h] = new
                    outs.append(jnp.sum(q_all[:, cols] * new, axis=0, keepdims=True))
                o_ref[h, pl.ds(half * ROWS, ROWS), :] = jnp.concatenate(outs, axis=0)
            return 0

        lax.fori_loop(0, heads, body, 0)

    def project_out(t, base):
        squares = jnp.zeros((pair_rows, 1), jnp.float32)
        gated = []
        for h in range(heads):
            o = o_ref[h]
            squares += jnp.sum(o * o, axis=1, keepdims=True)
            gated.append((o * onorm_ref[h:h + 1, :] * proj_ref[3, h, pl.ds(base, pair_rows), :]).astype(jnp.bfloat16))
        gated = jnp.concatenate(gated, axis=1)
        tile = 1024
        for c in range(width // tile):
            cols = pl.ds(c * tile, tile)
            w = wout_ref[:, :, cols].reshape(heads * dim, tile)
            y = jnp.dot(gated, w, preferred_element_type=jnp.float32)
            part_ref[pl.ds(2 * t, 2), :, cols] = y.reshape(2, ROWS, tile)
        part_ref[pl.ds(2 * t, 2), :, pl.ds(width, LANES)] = jnp.broadcast_to(squares, (pair_rows, LANES)).reshape(2, ROWS, LANES)

    for s in range(4):
        t = ring.order[s]
        base = pl.multiple_of(t * pair_rows, pair_rows)
        for c in [state_copy(s + 2, 0), state_copy(s + 2, 1)] if s < 2 else (late, caches)[s - 2]:
            c.start()
        for half in range(2):
            state_copy(s, half).wait()
        update(base)
        if s == 0:
            for h in range(heads):
                wout_copy(h).wait()
        if s == 1:
            total.far()
        if s == 2:
            total.next()
        if s == 3:
            total.previous()
            total.relay()
        project_out(t, base)
        total.to_mate(s)
    for c in wout2:
        c.start()
    total.own()

    inv = lax.rsqrt(acc_ref[3, :, pl.ds(width, 1)] / full_width + EPS)
    lin = acc_ref[3, :, pl.ds(0, width)] * inv
    mid = (alpha_ref[0] * gather_ref[ring.me] + beta_ref[0] * lin).astype(jnp.bfloat16).astype(jnp.float32)
    h2 = mid * lax.rsqrt(jnp.mean(mid * mid, axis=-1, keepdims=True) + EPS) * norm2_ref[...]
    h2 = h2.astype(jnp.bfloat16).astype(jnp.float32)
    own_ref[...] = h2
    gather_ref[ring.me] = h2
    gather_rows(ring, gather_ref)
    h2_ref[...] = gather_ref[...].reshape(h2_ref.shape).astype(h2_ref.dtype)
    ring.drain()
    for c in late + caches + wout2:
        c.wait()


def in_hbm(x):
    return pltpu.with_memory_space_constraint(x, pltpu.HBM)


def in_vmem(x):
    return pltpu.with_memory_space_constraint(x, pltpu.VMEM)


def first_sublayer(tp_size, slopes, cache_len, freq, norm_first, out_norm, norm_second, mix_alpha, mix_beta, hidden,
                   w_qkv, w_gate, lin_state, w_out_lin, w_attn, w_out_attn, k_cache, v_cache):
    batch, width = hidden.shape
    heads, dim = out_norm.shape
    blocks = batch // ROWS
    slots = w_attn.shape[0]
    chips = tp_size // 2
    f32, bf16 = jnp.float32, jnp.bfloat16
    part_width = width + LANES
    args = (slopes, cache_len, freq, norm_first.reshape(1, width), out_norm, norm_second.reshape(1, width), mix_alpha, mix_beta, hidden,
            w_qkv, w_gate, lin_state, w_out_lin, w_attn, w_out_attn, k_cache, v_cache)
    dma = pltpu.SemaphoreType.DMA
    return pl.pallas_call(
        functools.partial(first_kernel, chips, heads * dim * tp_size),
        out_shape=(pltpu.VMEM(lin_state.shape, f32),
                   pltpu.VMEM((slots, width, dim), bf16),
                   pltpu.VMEM((heads, dim, width), bf16),
                   pltpu.VMEM(k_cache.shape, k_cache.dtype),
                   pltpu.VMEM(v_cache.shape, v_cache.dtype),
                   pltpu.VMEM((batch, width), bf16),
                   pltpu.VMEM((ROWS, width), f32),
                   pltpu.VMEM((3, batch, dim), f32),
                   pltpu.VMEM((batch, ROWS, LANES), jnp.int32)),
        in_specs=[HBM] * len(args),
        out_specs=(VMEM,) * 9,
        scratch_shapes=[
            pltpu.SMEM((heads,), f32), pltpu.SMEM((batch,), jnp.int32), pltpu.VMEM((1, dim), f32), pltpu.VMEM((1, width), f32),
            pltpu.VMEM((heads, dim), f32), pltpu.VMEM((1, width), f32), pltpu.SMEM((2,), f32), pltpu.SMEM((2,), f32),
            pltpu.VMEM((batch, width), bf16),
            pltpu.VMEM((4, heads, batch, dim), f32),
            pltpu.VMEM((heads, 2 * ROWS, dim), f32),
            pltpu.VMEM((blocks, ROWS, part_width), f32),
            pltpu.VMEM((blocks, ROWS, width), f32),
            dma((9,)), dma((slots,)), dma((heads,)), dma((4, 2)), dma((4, 8)), dma((32,)), dma((32,)),
        ] + RowSum.scratch(chips, ROWS, part_width, half_of(part_width)),
        compiler_params=pltpu.CompilerParams(collective_id=0, has_side_effects=True, vmem_limit_bytes=VMEM_LIMIT),
        cost_estimate=pl.CostEstimate(flops=10 ** 11, transcendentals=0, bytes_accessed=10 ** 8),
        name="first_sublayer",
    )(*[in_hbm(x) for x in args])


def attention_kernel(len_ref, h2_ref, table_ref, pos_ref, watt_ref, k_ref, v_ref, wout_ref, state_ref,
                     k_out_hbm, v_out_hbm, state_out_hbm, part_ref, q_ref, kn_ref, vn_ref, att_ref, patch_ref, bulk_sem, patch_sem,
                     state_sem):
    batch, width = h2_ref.shape
    group = watt_ref.shape[0] - 2
    dim = watt_ref.shape[2]
    tmax = k_ref.shape[2]
    per = 8
    sub = 16
    blocks = batch // per

    def bulk(i, which):
        src, dst = ((k_ref, k_out_hbm), (v_ref, v_out_hbm))[which]
        rows = pl.ds(i * per, per)
        return pltpu.make_async_copy(src.at[rows], dst.at[rows], bulk_sem.at[i, which])

    def patch(b, which):
        dst = (k_out_hbm, v_out_hbm)[which]
        start = pl.multiple_of((len_ref[b] // sub) * sub, sub)
        return pltpu.make_async_copy(patch_ref.at[which, b], dst.at[b, 0, pl.ds(start, sub)], patch_sem.at[b, which])

    for i in range(blocks):
        for which in range(2):
            bulk(i, which).start()
    states = [pltpu.make_async_copy(state_ref.at[pl.ds(i * per, per)], state_out_hbm.at[pl.ds(i * per, per)], state_sem.at[i])
              for i in range(blocks)]
    for c in states:
        c.start()

    h2 = h2_ref[...]

    def turn(x):
        return (x * table_ref[0] + pltpu.roll(x, dim - dim // 4, 1) * table_ref[1] + pltpu.roll(x, dim // 4, 1) * table_ref[2])

    q_ref[...] = jnp.zeros_like(q_ref)
    for j in range(group):
        q_ref[:, j, :] = turn(jnp.dot(h2, watt_ref[j], preferred_element_type=jnp.float32))
    kn_ref[...] = turn(jnp.dot(h2, watt_ref[group], preferred_element_type=jnp.float32)).astype(jnp.bfloat16).astype(jnp.float32)
    vn_ref[...] = jnp.dot(h2, watt_ref[group + 1], preferred_element_type=jnp.float32).astype(jnp.bfloat16).astype(jnp.float32)

    rows16 = lax.broadcasted_iota(jnp.int32, (sub, dim), 0)
    flat = per * ROWS
    cols = lax.broadcasted_iota(jnp.int32, (flat, tmax), 1)
    scale = dim ** -0.5

    def spread(rows):
        return jnp.concatenate([jnp.broadcast_to(rows[r:r + 1, :], (ROWS, dim)) for r in range(per)], axis=0)

    def block(i, _):
        base = pl.multiple_of(i * per, per)
        news = [kn_ref[pl.ds(base, per), :], vn_ref[pl.ds(base, per), :]]
        for r in range(per):
            b = base + r
            pos = len_ref[b]
            start = pl.multiple_of((pos // sub) * sub, sub)
            for which, ref in ((0, k_ref), (1, v_ref)):
                old = ref[b, 0, pl.ds(start, sub), :].astype(jnp.float32)
                patch_ref[which, b] = jnp.where(rows16 == pos - start, news[which][r:r + 1, :], old).astype(jnp.bfloat16)
        q = q_ref[pl.ds(base, per)].reshape(flat, dim)
        q_bf = q.astype(jnp.bfloat16)
        s_new = jnp.sum(q_bf.astype(jnp.float32) * spread(news[0]), axis=1, keepdims=True)
        scores = [lax.dot_general(q_bf[r * ROWS:(r + 1) * ROWS], k_ref[base + r, 0], (((1,), (1,)), ((), ())),
                                  preferred_element_type=jnp.float32) for r in range(per)]
        s = jnp.concatenate(scores, axis=0)
        pos = pos_ref[pl.ds(base, per)].reshape(flat, LANES)
        pos = jnp.concatenate([pos] * (tmax // LANES), axis=1)
        at_pos = cols == pos
        s = jnp.where(at_pos, s_new, s) * scale
        s = jnp.where(cols <= pos, s, -jnp.inf)
        e = jnp.exp(s - jnp.max(s, axis=1, keepdims=True))
        p = (e * (1.0 / jnp.sum(e, axis=1, keepdims=True))).astype(jnp.bfloat16).astype(jnp.float32)
        p_new = jnp.sum(jnp.where(at_pos, p, 0.0), axis=1, keepdims=True)
        p_old = jnp.where(at_pos, 0.0, p).astype(jnp.bfloat16)
        outs = [jnp.dot(p_old[r * ROWS:(r + 1) * ROWS], v_ref[base + r, 0], preferred_element_type=jnp.float32)
                for r in range(per)]
        att = jnp.concatenate(outs, axis=0) + p_new * spread(news[1])
        att_ref[pl.ds(base, per)] = att.reshape(per, ROWS, dim)
        for which in range(2):
            bulk(i, which).wait()
        for r in range(per):
            for which in range(2):
                patch(base + r, which).start()
        return 0

    lax.fori_loop(0, blocks, block, 0)
    rows = jnp.concatenate([att_ref[:, j, :] for j in range(group)], axis=1).astype(jnp.bfloat16)
    tile = 1024
    for c in range(width // tile):
        cs = pl.ds(c * tile, tile)
        piece = jnp.dot(rows, wout_ref[:, :, cs].reshape(group * dim, tile), preferred_element_type=jnp.float32)
        part_ref[:, :, cs] = piece.reshape(batch // ROWS, ROWS, tile)

    def finish(b, _):
        for which in range(2):
            patch(b, which).wait()
        return 0

    lax.fori_loop(0, batch, finish, 0)
    for c in states:
        c.wait()


def attention(cache_len, h2, w_attn, tables, positions, k_cache, v_cache, w_out, state):
    batch, width = h2.shape
    _, _, tmax, dim = k_cache.shape
    slots = w_attn.shape[0]
    blocks = batch // ROWS
    return pl.pallas_call(
        attention_kernel,
        out_shape=(pltpu.HBM(k_cache.shape, k_cache.dtype), pltpu.HBM(v_cache.shape, v_cache.dtype),
                   pltpu.HBM(state.shape, state.dtype),
                   pltpu.VMEM((blocks, ROWS, width), jnp.float32)),
        in_specs=[SMEM] + [VMEM] * 8,
        out_specs=(HBM, HBM, HBM, VMEM),
        scratch_shapes=[
            pltpu.VMEM((batch, ROWS, dim), jnp.float32),
            pltpu.VMEM((batch, dim), jnp.float32),
            pltpu.VMEM((batch, dim), jnp.float32),
            pltpu.VMEM((batch, ROWS, dim), jnp.float32),
            pltpu.VMEM((2, batch, 16, dim), k_cache.dtype),
            pltpu.SemaphoreType.DMA((batch // 8, 2)),
            pltpu.SemaphoreType.DMA((batch, 2)),
            pltpu.SemaphoreType.DMA((batch // 8,)),
        ],
        compiler_params=pltpu.CompilerParams(vmem_limit_bytes=VMEM_LIMIT),
        cost_estimate=pl.CostEstimate(flops=2 * batch * width * dim * slots * 2, transcendentals=0,
                                      bytes_accessed=4 * k_cache.size * 2),
        name="attention",
    )(cache_len, *[in_vmem(x) for x in (h2, tables, positions, w_attn, k_cache, v_cache, w_out, state)])


def rotary_freq(dim):
    rot = dim // 2
    half = rot // 2
    freq = ROPE_BASE ** (-2.0 * np.arange(half) / rot)
    return jnp.asarray(np.concatenate([freq, freq, np.zeros(dim - rot)])[None, :], jnp.float32)


def solution(mesh):
    tp_size = mesh.shape['tp']
    row_spec = P('dp', None)
    cache_spec = P('dp', 'tp', None, None)
    in_specs = (row_spec, P('dp'), cache_spec, cache_spec, cache_spec, P(None), P(None, None, 'tp', None),
                P(None, 'tp', None), P('tp'), P('tp', None), P('tp', None, None), P(None),
                P(None, 'tp', None, None), P('tp', None, None), P(None), P(None))
    out_specs = (row_spec, cache_spec, cache_spec, cache_spec)

    def local_step(hidden, cache_len, lin_state, k_cache, v_cache, norm_first, w_qkv, w_gate, slopes, out_norm,
                   w_out_lin, norm_second, w_attn, w_out_attn, mix_alpha, mix_beta):
        width = hidden.shape[1]
        dim = k_cache.shape[3]
        w_heads = w_attn.transpose(1, 2, 0, 3).reshape(w_attn.shape[2], width, dim)
        state, w_heads, w_out, keys, values, h2, h2_own, tables, positions = first_sublayer(
            tp_size, slopes, cache_len, rotary_freq(dim), norm_first, out_norm, norm_second, mix_alpha, mix_beta, hidden,
            w_qkv.transpose(1, 2, 0, 3), w_gate.transpose(1, 0, 2), lin_state, w_out_lin, w_heads, w_out_attn, k_cache, v_cache)
        k_out, v_out, state_out, part = attention(cache_len, h2, w_heads, tables, positions, keys, values, w_out, state)
        hidden_out = second_sum(tp_size, part, h2_own, mix_alpha, mix_beta)
        return hidden_out, state_out, k_out, v_out

    return jax.shard_map(local_step, mesh=mesh, in_specs=in_specs, out_specs=out_specs, check_vma=False)
```
